512 devices in a mesh: groups: 2 (over y), seq: 128 (over z, x), tp: 2 (over core).
Axes of the slice: x: 8, y: 2, z: 16, core: 2. Of those that a mesh axis runs over, the one named last changes fastest.
The devices are a block of a 8x8x16 slice.
Arguments:
- stream: bfloat16 [2048, 6144], P(('groups', 'seq'), 'tp'), parts along dimension 0, may hold values from -6 to 6
- queries: bfloat16 [2048, 6144], P(('groups', 'seq'), 'tp'), parts along dimension 0, may hold values from -6 to 6
- key_rows: bfloat16 [2048, 1024], P(('groups', 'seq'), 'tp'), parts along dimension 0, may hold values from -6 to 6
- value_rows: bfloat16 [2048, 1024], P(('groups', 'seq'), 'tp'), parts along dimension 0, may hold values from -6 to 6
- routes: int32 [2048, 2], P(('groups', 'seq')), parts along dimension 0, may hold values from 0 to 3, all different within a row; in each aligned block of 8 rows (0 to 7, 8 to 15, ...) at most 4 rows name the same one
- seq_length: int32 [2], P('groups'), parts along dimension 0, may hold values from 256 to 1024
- norm_gain: float32 [6144], P('tp'), may hold values from 0.25 to 1.75
- router: float32 [6144, 4], P('tp'), may hold values from -0.078125 to 0.078125
- w_up: bfloat16 [6144, 32768], P('tp', 'seq'), may hold values from -0.078125 to 0.078125
- w_down: bfloat16 [32768, 6144], P('seq', 'tp'), may hold values from -0.0625 to 0.0625
- final_gain: float32 [6144], P('tp'), may hold values from 0.25 to 1.75
- value_weight: float32 [6144], P('tp'), may hold values from -0.078125 to 0.078125
- value_bias: float32 [1], replicated, may hold values from -3 to 3
Outputs:
- layer_out: bfloat16 [2048, 6144], P(('groups', 'seq'), 'tp'), parts along dimension 0
- values: float32 [2048], P(('groups', 'seq')), parts along dimension 0
The draws below stay inside these ranges and needn't reach their ends.
There are 2 independent parts, one for each index of `groups`. The reference program is written for one: setup_inputs(seed, part) draws one part's arguments, and reference() takes and returns one part's arrays. A program takes and returns all parts, laid end to end along the dimension named above; an argument that names none is the same for every part. Nothing has to cross between parts.
Inputs may be any that keep to these rules, and one draw needn't show every extreme that they name: `routes`: each row names two different experts; among the rows on one device no expert is named more than 4 times, and some device's rows name some expert exactly 4 times.
All inputs are finite; a program needn't handle non-finite values.
Results may differ from the reference program's by a relative error of at most 0.01.
Values may be sent and summed in bfloat16 or wider, within the bound.
A program may use at most 64 MiB of HBM per device.

```python
import math
import jax
import jax.numpy as jnp
import numpy as np
from jax import lax

D = 6144
HQ = 48
KVH = 8
HD = 128
EXPERTS = 4
F = 8192
LEN_DEV = 8
LENGTH = 1024
CAP = 4
N_SEQ = 128


def draw_queries(key, part):
    values = jnp.clip(1.5 * jax.random.normal(jax.random.fold_in(key, 11), (LENGTH, HQ * HD), jnp.float32), -6.0, 6.0)
    return values.astype(jnp.bfloat16)


def draw_key_rows(key, part):
    values = jnp.clip(jax.random.normal(jax.random.fold_in(key, 12), (LENGTH, KVH * HD), jnp.float32), -6.0, 6.0)
    return values.astype(jnp.bfloat16)


def block_scale(stream_key, shape, split, least, top_value):
    gain = 1.0
    for position, shards_of in split:
        heights = jax.random.uniform(jax.random.fold_in(jax.random.fold_in(stream_key, 6), position), (shards_of,), jnp.float32, least / len(split), top_value / len(split))
        gain = gain * jnp.repeat(jnp.exp(heights), shape[position] // shards_of).reshape((-1,) + (1,) * (len(shape) - 1 - position))
    return gain


def shared_out(rng, own, number, rows, count, top, reach, lean):
    sequence = jax.random.permutation(rng, count)
    heavy_load, ordinary = shares(count, rows * top, reach, lean, True), shares(count, rows * top, reach, lean, False)
    places = jnp.arange(count)

    def named(lengths, rotation):
        used = int((lengths > 0).sum())
        fixed = max(1, used // 4)
        passed = fixed + (places - fixed + rotation * (used - fixed)) % max(1, count - fixed)
        return jnp.zeros((count,), jnp.int32).at[sequence[jnp.where(places < fixed, places, passed)]].set(jnp.asarray(lengths, jnp.int32))

    lengths = jnp.where(number % 4 == 0, named(heavy_load, number // 4), named(ordinary, number - number // 4 - 1))
    mixed = jax.random.permutation(jax.random.fold_in(own, 3), count)
    giver, taker = mixed[0:count // 2 * 2:2], mixed[1:count // 2 * 2:2]
    slack = jnp.minimum(lengths[giver] - 1, reach - lengths[taker]) // 2
    slack = jnp.where((giver == sequence[0]) | (taker == sequence[0]) | (lengths[taker] == 0), 0, jnp.maximum(slack, 0))
    passed = jax.random.randint(jax.random.fold_in(own, 4), (count // 2,), 0, 1 << 20) % (slack + 1)
    lengths = lengths.at[giver].add(-passed).at[taker].add(passed)
    members = jnp.searchsorted(jnp.cumsum(lengths), jnp.arange(rows * top), side="right").astype(jnp.int32)
    grid = members.reshape(top, rows).T
    grid = grid[jax.random.permutation(jax.random.fold_in(own, 1), rows)]
    rotation = jax.random.randint(jax.random.fold_in(own, 2), (rows, 1), 0, top)
    return jnp.take_along_axis(grid, (jnp.arange(top)[None, :] + rotation) % top, axis=1)


def shares(count, total, most, lean, full):
    portions = [(1 << 20) // math.isqrt(grade ** lean) + 1 for grade in range(1, count + 1)]
    largest = most if full else min(most, max(-(-total // count), total * portions[0] // sum(portions)))
    least = 1 if total - largest >= count - 1 else 0
    counts, spare = [largest] + [least] * (count - 1), total - largest - least * (count - 1)
    while spare > 0:
        movable = [i for i in range(1, count) if counts[i] < largest] or [i for i in range(1, count) if counts[i] < most]
        mass, remaining = sum([portions[i] for i in movable]), spare
        for i in movable:
            addition = min(most - counts[i], max(1, remaining * portions[i] // mass), spare)
            counts[i] = counts[i] + addition
            spare = spare - addition
    return np.array(counts)


def noise(own_key, extent, width, most, shards=(), kind=jnp.bfloat16):
    drawn = width * jax.random.normal(own_key, extent, jnp.float32)
    if shards:
        drawn = drawn * block_scale(own_key, extent, shards, -0.22, 0.18)
    return jnp.clip(drawn, -most, most).astype(kind)


def setup_inputs(seed: int = 0, part: int = 0) -> dict:
    arg_keys = jax.random.split(jax.random.key(seed), 14)
    part_keys = jax.random.split(jax.random.fold_in(arg_keys[13], part), 14)
    stream = noise(part_keys[0], (LENGTH, D), 1.0, 6.0, ((0, 128), (1, 2)))
    queries = draw_queries(jax.random.fold_in(jax.random.fold_in(arg_keys[13], part), 71), part)
    key_rows = draw_key_rows(jax.random.fold_in(jax.random.fold_in(arg_keys[13], part), 71), part)
    value_rows = noise(part_keys[3], (LENGTH, KVH * HD), 1.0, 6.0, ((0, 128), (1, 2)))
    routes_keys = jax.random.split(jax.random.fold_in(part_keys[4], 1), LENGTH // LEN_DEV)
    routes_turns = jax.random.permutation(jax.random.fold_in(part_keys[4], 3), LENGTH // LEN_DEV)
    routes = jax.vmap(lambda own, number: shared_out(jax.random.fold_in(part_keys[4], 2), own, number, LEN_DEV, EXPERTS, 2, CAP, 2))(routes_keys, routes_turns).reshape((LENGTH, 2))
    seq_length = jax.random.randint(part_keys[5], (1,), LENGTH // 4, LENGTH + 1).astype(jnp.int32)
    norm_gain = jnp.clip(1.0 + 0.15 * jax.random.normal(arg_keys[6], (D,), jnp.float32), 0.25, 1.75)
    router = noise(arg_keys[7], (D, EXPERTS), D ** -0.5, 0.078125, ((0, 2),), jnp.float32)
    w_up = noise(arg_keys[8], (D, EXPERTS * F), D ** -0.5, 0.078125, ((0, 2), (1, 128)))
    w_down = noise(arg_keys[9], (EXPERTS * F, D), F ** -0.5, 0.0625, ((0, 128), (1, 2)))
    final_gain = jnp.clip(1.0 + 0.15 * jax.random.normal(arg_keys[10], (D,), jnp.float32), 0.25, 1.75)
    value_weight = noise(arg_keys[11], (D,), D ** -0.5, 0.078125, ((0, 2),), jnp.float32)
    value_bias = noise(arg_keys[12], (1,), 1.0, 3.0, (), jnp.float32)
    return dict(stream=stream, queries=queries, key_rows=key_rows, value_rows=value_rows, routes=routes, seq_length=seq_length, norm_gain=norm_gain, router=router, w_up=w_up, w_down=w_down, final_gain=final_gain, value_weight=value_weight, value_bias=value_bias)


eps = 1e-05

def attention(queries, key_rows, value_rows, seq_limit):
    per_group = HQ // KVH
    positions = jnp.arange(LENGTH, dtype=jnp.int32)
    allowed = (positions[None, :] <= positions[:, None]) & (positions[None, :] < seq_limit)
    q_heads = queries.reshape(LENGTH, KVH, per_group, HD).transpose(1, 2, 0, 3)
    k_heads = key_rows.reshape(LENGTH, KVH, HD).transpose(1, 0, 2)
    v_heads = value_rows.reshape(LENGTH, KVH, HD).transpose(1, 0, 2)

    def one_head(triple):
        q_one, k_one, v_one = triple
        scores = jnp.einsum('gqd,cd->gqc', q_one.astype(jnp.float32), k_one.astype(jnp.float32)) / math.sqrt(HD)
        scores = jnp.where(allowed, scores, -jnp.inf)
        top_score = lax.optimization_barrier(jnp.max(scores, axis=-1, keepdims=True))
        expo = jnp.where(allowed, jnp.exp(scores - top_score), 0.0)
        rounded = lax.optimization_barrier(expo.astype(jnp.bfloat16))
        numer = jnp.einsum('gqc,cd->gqd', rounded.astype(jnp.float32), v_one.astype(jnp.float32))
        return numer / lax.optimization_barrier(jnp.sum(expo, axis=-1))[..., None]
    heads = lax.map(one_head, (q_heads, k_heads, v_heads))
    return heads.transpose(2, 0, 1, 3).reshape(LENGTH, HQ * HD)

def reference(stream, queries, key_rows, value_rows, routes, seq_length, norm_gain, router, w_up, w_down, final_gain, value_weight, value_bias):
    seq_limit = seq_length[0]
    hidden = stream.astype(jnp.float32) + attention(queries, key_rows, value_rows, seq_limit)
    normed = hidden * lax.rsqrt(lax.optimization_barrier(jnp.mean(hidden * hidden, axis=1, keepdims=True)) + eps) * norm_gain
    normed_half = normed.astype(jnp.bfloat16)
    logits = jnp.dot(normed, router, precision=lax.Precision.HIGHEST)
    chosen = (routes[:, :, None] == jnp.arange(EXPERTS, dtype=jnp.int32)).astype(jnp.float32)
    picked = lax.optimization_barrier(jnp.sum(chosen * logits[:, None, :], axis=2))
    gates = jax.nn.sigmoid(picked - picked[:, ::-1])
    coeffs = lax.optimization_barrier(jnp.sum(chosen * gates[:, :, None], axis=1))
    owners = N_SEQ // EXPERTS
    block = F // owners
    mixed = jnp.zeros((LENGTH, D), jnp.float32)
    for expert in range(EXPERTS):
        up_proj = jnp.dot(normed_half, w_up[:, expert * F:(expert + 1) * F], preferred_element_type=jnp.float32)
        active = jax.nn.silu(up_proj).astype(jnp.bfloat16)
        down_rows = w_down[expert * F:(expert + 1) * F]

        def add_block(total, index):
            act_part = lax.dynamic_slice_in_dim(active, index * block, block, 1)
            weight_part = lax.dynamic_slice_in_dim(down_rows, index * block, block, 0)
            piece = jnp.dot(act_part, weight_part, preferred_element_type=jnp.float32).astype(jnp.bfloat16)
            return (total + lax.optimization_barrier(piece).astype(jnp.float32), None)
        expert_out, _ = lax.scan(add_block, jnp.zeros((LENGTH, D), jnp.float32), jnp.arange(owners, dtype=jnp.int32))
        mixed = mixed + coeffs[:, expert:expert + 1] * expert_out
    final = hidden + mixed
    mean_sq = lax.optimization_barrier(jnp.mean(final * final, axis=1))
    estimate = lax.optimization_barrier(jnp.sum(final * final_gain * value_weight, axis=1)) * lax.rsqrt(mean_sq + eps) + value_bias[0]
    positions = jnp.arange(LENGTH, dtype=jnp.int32)
    estimate = jnp.where(positions < seq_limit, estimate, 0.0)
    return (final.astype(jnp.bfloat16), estimate)
```

```python
import functools
import math

import jax
import jax.numpy as jnp
from jax import lax
from jax.experimental import pallas as pl
from jax.experimental.pallas import tpu as pltpu
from jax.sharding import Mesh
from jax.sharding import PartitionSpec as P

HD = 128
EXPERTS = 4
META = 128
SEQ = ("z", "x")
GROUPS_SEQ = ("groups", "z", "x")
eps = 1e-05
masked = -1e30
f32 = jnp.float32
bf16 = jnp.bfloat16


def lane_sum(a):
    return jnp.sum(a, axis=1, keepdims=True)


def kernel(
    dims,
    queries,
    key_rows,
    value_rows,
    stream,
    routes,
    seq_length,
    norm_gain,
    router,
    w_up_hbm,
    w_down_hbm,
    value_gain,
    value_bias,
    layer_out,
    values,
    kv,
    rows_z,
    rows_x,
    hidden,
    w_up,
    w_down,
    stats,
    stats_in,
    ups,
    ups_in,
    acts,
    parts,
    sums_r,
    sums_l,
    recv_r,
    recv_l,
    sums_z,
    recv_z,
    local_sem,
    zsend,
    xsend,
    zrecv,
    xrecv,
    tsend,
    trecv,
    usend,
    urecv,
):
    nz, nx, full_width = dims
    units, hops = nz // 2, nx // 2
    z, x, t = lax.axis_index("z"), lax.axis_index("x"), lax.axis_index("tp")
    up, down = {"z": lax.rem(z + 1, nz)}, {"z": lax.rem(z + nz - 1, nz)}
    right, left = {"x": lax.rem(x + 1, nx)}, {"x": lax.rem(x + nx - 1, nx)}
    twin = {"tp": 1 - t}
    count, width = stream.shape
    kv_width = key_rows.shape[1]

    def remote(src, dst, send, recv, to):
        return pltpu.make_async_remote_copy(
            src_ref=src, dst_ref=dst, send_sem=send, recv_sem=recv, device_id=to,
            device_id_type=pl.DeviceIdType.MESH,
        )

    key_copy = pltpu.make_async_copy(key_rows, kv.at[0, x, 0, :, pl.ds(0, kv_width)], local_sem.at[0])
    value_copy = pltpu.make_async_copy(
        value_rows, kv.at[0, x, 0, :, pl.ds(kv_width, kv_width)], local_sem.at[1]
    )
    up_copy = pltpu.make_async_copy(w_up_hbm, w_up, local_sem.at[2])
    down_copy = pltpu.make_async_copy(w_down_hbm, w_down, local_sem.at[3])
    key_copy.start()
    value_copy.start()
    up_copy.start()
    down_copy.start()
    barrier = pltpu.get_barrier_semaphore()
    for peer in (up, down, right, left, twin):
        pl.semaphore_signal(barrier, inc=1, device_id=peer, device_id_type=pl.DeviceIdType.MESH)
    key_copy.wait()
    value_copy.wait()
    pl.semaphore_wait(barrier, 5)

    def gather(phase, z_at, x_at, chosen, finish):
        def z_copy(way, u):
            if way == 0:
                return remote(z_at(u - 1, 0), z_at(u, 0), zsend.at[0, u], zrecv.at[phase, 0, u], down)
            return remote(z_at(u - 1, 1), z_at(u, 1), zsend.at[1, u], zrecv.at[phase, 1, u], up)

        def z_first():
            return remote(z_at(0, 0), z_at(0, 1), zsend.at[1, 0], zrecv.at[phase, 1, 0], up)

        def x_copy(way, u, h):
            back = nx - (h - 1) if way == 0 else h - 1
            at = x_at(u, lax.rem(x + back, nx))
            return remote(
                at, at, xsend.at[way, u, h - 1], xrecv.at[phase, way, u, h - 1], right if way == 0 else left
            )

        def x_arrival(way, u, h):
            back = nx - h if way == 0 else h
            at = x_at(u, lax.rem(x + back, nx))
            return remote(
                at, at, xsend.at[way, u, h - 1], xrecv.at[phase, way, u, h - 1], right if way == 0 else left
            )

        z_first().start()
        z_copy(0, 1).start()

        def slot(step, carry):
            @pl.when(step < units)
            def _():
                u = step

                @pl.when(u > 0)
                def _():
                    z_copy(0, u).wait_recv()
                    z_copy(1, u).wait_recv()

                @pl.when(u == 0)
                def _():
                    z_first().wait_recv()

                @pl.when(u < units - 1)
                def _():
                    z_copy(1, u + 1).start()

                @pl.when((u > 0) & (u < units - 1))
                def _():
                    z_copy(0, u + 1).start()

                chosen(u)
                x_copy(0, u, 1).start()
                x_copy(1, u, 1).start()

            for h in range(1, hops):
                u = step - h

                @pl.when((u >= 0) & (u < units))
                def _():
                    for way in (0, 1):
                        x_arrival(way, u, h).wait_recv()
                        if h < hops - 1:
                            x_copy(way, u, h + 1).start()
                        else:

                            @pl.when(lax.rem(u, 2) == way)
                            def _():
                                x_copy(way, u, h + 1).start()

            u = step - hops

            @pl.when(u >= 0)
            def _():
                for way in (0, 1):

                    @pl.when(lax.rem(u, 2) == way)
                    def _():
                        x_arrival(way, u, hops).wait_recv()

                finish(u)

            return carry

        lax.fori_loop(0, units + hops, slot, 0)

        def drain(u, carry):
            @pl.when(u > 0)
            def _():
                z_copy(0, u).wait_send()
                z_copy(1, u).wait_send()

            @pl.when(u == 0)
            def _():
                z_first().wait_send()

            for way in (0, 1):
                for h in range(1, hops):
                    x_copy(way, u, h).wait_send()

                @pl.when(lax.rem(u, 2) == way)
                def _():
                    x_copy(way, u, hops).wait_send()

            return carry

        lax.fori_loop(0, units, drain, 0)

    gather(
        0,
        lambda u, half: kv.at[u, x, half],
        lambda u, source: kv.at[u, source],
        lambda u: None,
        lambda u: None,
    )

    heads = kv_width // HD
    per_group = width // kv_width
    keys = nz * nx * count
    limit = seq_length[0]
    n = lax.broadcasted_iota(jnp.int32, (1, keys), 1)
    per_unit = nx * 2 * count
    key_u, rest = n // per_unit, lax.rem(n, per_unit)
    key_x, rest = rest // (2 * count), lax.rem(rest, 2 * count)
    key_half, key_r = rest // count, lax.rem(rest, count)
    key_z = lax.rem(jnp.where(key_half == 0, z + key_u, z - key_u - 1 + nz), nz)
    key_pos = (key_z * nx + key_x) * count + key_r
    token = lax.broadcasted_iota(jnp.int32, (count, 1), 0)
    my_pos = (z * nx + x) * count + token
    ok = (key_pos <= my_pos) & (key_pos < limit)
    allowed = jnp.concatenate([ok.astype(f32)] * per_group, axis=0) > 0.5
    for head in range(heads):
        q = jnp.concatenate(
            [
                queries[:, (head * per_group + j) * HD : (head * per_group + j + 1) * HD].astype(f32)
                for j in range(per_group)
            ],
            axis=0,
        ).astype(bf16)
        k = kv[:, :, :, :, head * HD : (head + 1) * HD].reshape(keys, HD)
        v = kv[:, :, :, :, kv_width + head * HD : kv_width + (head + 1) * HD].reshape(keys, HD)
        s = lax.dot_general(q, k, (((1,), (1,)), ((), ())), preferred_element_type=f32) * (1.0 / math.sqrt(HD))
        s = jnp.where(allowed, s, masked)
        p = jnp.where(allowed, jnp.exp(s - jnp.max(s, axis=1, keepdims=True)), 0.0)
        o = jnp.dot(p.astype(bf16), v, preferred_element_type=f32) / lane_sum(p)
        for j in range(per_group):
            at = slice((head * per_group + j) * HD, (head * per_group + j + 1) * HD)
            hidden[:, at] = stream[:, at].astype(f32) + o[j * count : (j + 1) * count]

    def both(index, message):
        stats[index] = message
        copy = remote(stats.at[index], stats_in.at[index], tsend.at[index], trecv.at[index], twin)
        copy.start()
        copy.wait()
        return message + stats_in[index]

    lane = lax.broadcasted_iota(jnp.int32, (count, META), 1)
    row = lax.broadcasted_iota(jnp.int32, (count, META), 0)
    h_all = hidden[...]
    gained = h_all * norm_gain[...]
    raw = jnp.dot(gained, router[...], preferred_element_type=f32, precision=lax.Precision.HIGHEST)
    message = jnp.where(lane == EXPERTS, lane_sum(h_all * h_all), 0.0)
    for e in range(EXPERTS):
        message = jnp.where(lane == e, raw[:, e : e + 1], message)
    total = both(0, message)
    sq = lane_sum(jnp.where(lane == EXPERTS, total, 0.0))
    scale = lax.rsqrt(sq / full_width + eps)
    logits = total * scale
    first, second = routes[:, 0:1], routes[:, 1:2]
    hit_a, hit_b = lane == first, lane == second
    gap = lane_sum(jnp.where(hit_a, logits, 0.0)) - lane_sum(jnp.where(hit_b, logits, 0.0))
    gate_a, gate_b = 1.0 / (1.0 + jnp.exp(-gap)), 1.0 / (1.0 + jnp.exp(gap))
    hits = jnp.where(hit_a | hit_b, 1.0, 0.0)
    rank = jnp.zeros((count, META), f32)
    for i in range(count - 1):
        rank = rank + jnp.where(row > i, jnp.broadcast_to(hits[i : i + 1], (count, META)), 0.0)
    place = jnp.where(hits > 0.5, rank + 1.0, 0.0)
    meta = place
    for base, hit, gate in ((0, first, gate_a), (0, second, gate_b)):
        high = gate.astype(bf16).astype(f32)
        meta = jnp.where(lane == hit + EXPERTS, high, meta)
        meta = jnp.where(lane == hit + 2 * EXPERTS, gate - high, meta)
    rows_z[0, 0, :, :width] = (gained * scale).astype(bf16)
    rows_z[0, 0, :, width:] = meta.astype(bf16)

    my_expert = z // (nz // EXPERTS)

    def column(info, which):
        return lane_sum(jnp.where(lane == which * EXPERTS + my_expert, info, 0.0))

    slots = count // 2

    def choose(u):
        out = jnp.zeros((count, width), f32)
        for half in (0, 1):
            block = rows_z[u, half].astype(f32)
            places = jnp.broadcast_to(column(block[:, width:], 0), (count, META))
            for i in range(count):
                want = jnp.broadcast_to(places[i : i + 1], (count, META)) + (slots * half)
                mine = (row + 1).astype(f32) == want
                mine = jnp.where(mine & (want > slots * half + 0.5), 1.0, 0.0)
                out = out + mine[:, 0:1] * block[i : i + 1, :width]
        rows_x[u, x] = out.astype(bf16)

    def ups_copy(u):
        return remote(ups.at[u], ups_in.at[u], usend.at[u], urecv.at[u], twin)

    def activate(u):
        ups_copy(u).wait_recv()
        v = ups[u] + ups_in[u]
        acts[u] = (v / (1.0 + jnp.exp(-v))).astype(bf16)

    def project(u):
        @pl.when(u == 0)
        def _():
            up_copy.wait()

        got = rows_x[u].reshape(nx * count, width)
        ups[u] = jnp.dot(got, w_up[...], preferred_element_type=f32)
        ups_copy(u).start()

    gather(1, lambda u, half: rows_z.at[u, half], lambda u, source: rows_x.at[u, source], choose, project)
    down_copy.wait()

    def act_all(u, carry):
        activate(u)
        ups_copy(u).wait_send()
        return carry

    lax.fori_loop(0, units, act_all, 0)

    def r_copy(way, u, k, src):
        return remote(
            src,
            (recv_r if way == 0 else recv_l).at[u, k],
            xsend.at[way, u, k],
            xrecv.at[2, way, u, k],
            right if way == 0 else left,
        )

    def own(way, u, k):
        ahead = hops - k
        return parts.at[u, lax.rem(x + (ahead if way == 0 else nx - ahead), nx)]

    def zr_copy(way, u):
        return remote(
            sums_z.at[way, u], recv_z.at[way, u], zsend.at[way, u], zrecv.at[2, way, u], up if way == 0 else down
        )

    def home(u):
        both_ways = recv_r[u, hops - 1].astype(f32) + recv_l[u, hops - 1].astype(f32)
        done = parts[u, x].astype(f32) + both_ways
        for half in (0, 1):
            info = rows_z[u, half, :, width:].astype(f32)
            places = column(info, 0)
            gate = column(info, 1) + column(info, 2)
            mix = jnp.zeros((count, width), f32)
            for i in range(slots):
                weight = jnp.where(places == float(i + 1), gate, 0.0)
                mix = mix + weight * done[half * slots + i : half * slots + i + 1]
            sums_z[half, u] = mix.astype(bf16)

            @pl.when(u < units - 1)
            def _():
                zr_copy(half, u + 1).wait_recv()
                total = mix + recv_z[half, u + 1].astype(f32)
                sums_z[half, u] = total.astype(bf16)

                if half == 0:

                    @pl.when(u == 0)
                    def _():
                        hidden[...] = hidden[...] + total

            if half == 0:

                @pl.when(u > 0)
                def _():
                    zr_copy(0, u).start()

            else:
                zr_copy(1, u).start()

    def scatter(step, carry):
        @pl.when(step < units)
        def _():
            u = units - 1 - step
            made = jnp.dot(acts[u], w_down[...], preferred_element_type=f32)
            for d in range(nx):
                parts[u, d] = made[d * count : (d + 1) * count].astype(bf16)
            for way in (0, 1):

                @pl.when(lax.rem(u, 2) == way)
                def _():
                    r_copy(way, u, 0, own(way, u, 0)).start()

        for k in range(1, hops):
            u = units - 1 - (step - k)

            @pl.when((u >= 0) & (u < units))
            def _():
                for way, recv, sums in ((0, recv_r, sums_r), (1, recv_l, sums_l)):

                    def add():
                        r_copy(way, u, k - 1, own(way, u, k - 1)).wait_recv()
                        total = recv[u, k - 1].astype(f32) + own(way, u, k)[...].astype(f32)
                        sums[u, k] = total.astype(bf16)
                        r_copy(way, u, k, sums.at[u, k]).start()

                    if k > 1:
                        add()
                    else:
                        pl.when(lax.rem(u, 2) == way)(add)

                        @pl.when(lax.rem(u, 2) != way)
                        def _():
                            r_copy(way, u, k, own(way, u, k)).start()

        u = units - 1 - (step - hops)

        @pl.when(u < units)
        def _():
            for way in (0, 1):
                r_copy(way, u, hops - 1, own(way, u, hops - 1)).wait_recv()
            home(u)

        return carry

    lax.fori_loop(0, units + hops, scatter, 0)
    zr_copy(1, 0).wait_recv()
    out = hidden[...] + recv_z[1, 0].astype(f32)
    layer_out[...] = out.astype(bf16)
    message = jnp.where(lane == 0, lane_sum(out * out), 0.0)
    message = jnp.where(lane == 1, lane_sum(out * value_gain[...]), message)
    total = both(1, message)
    estimate = total[:, 1:2] * lax.rsqrt(total[:, 0:1] / full_width + eps) + value_bias[0]
    values[...] = jnp.broadcast_to(jnp.where(my_pos < limit, estimate, 0.0), (count, META))

    def drain(u, carry):
        @pl.when(u > 0)
        def _():
            zr_copy(0, u).wait_send()

        zr_copy(1, u).wait_send()
        for way in (0, 1):

            @pl.when(lax.rem(u, 2) == way)
            def _():
                r_copy(way, u, 0, own(way, u, 0)).wait_send()

            for k in range(1, hops):
                r_copy(way, u, k, own(way, u, k)).wait_send()
        return carry

    lax.fori_loop(0, units, drain, 0)


def on_device(dims, *args):
    (stream, queries, key_rows, value_rows, routes, seq_length, norm_gain, router) = args[:8]
    (w_up, w_down, final_gain, value_weight, value_bias) = args[8:]
    nz, nx, _ = dims
    units, hops = nz // 2, nx // 2
    count, width = stream.shape
    hid = w_up.shape[1]
    vmem, smem, far = (
        pl.BlockSpec(memory_space=pltpu.VMEM),
        pl.BlockSpec(memory_space=pltpu.SMEM),
        pl.BlockSpec(memory_space=pl.ANY),
    )
    dma = pltpu.SemaphoreType.DMA
    layer_out, values = pl.pallas_call(
        functools.partial(kernel, dims),
        out_shape=(
            jax.ShapeDtypeStruct((count, width), bf16),
            jax.ShapeDtypeStruct((count, META), f32),
        ),
        in_specs=[vmem, far, far, vmem, vmem, smem, vmem, vmem, far, far, vmem, smem],
        out_specs=(vmem, vmem),
        scratch_shapes=[
            pltpu.VMEM((units, nx, 2, count, 2 * key_rows.shape[1]), bf16),
            pltpu.VMEM((units, 2, count, width + META), bf16),
            pltpu.VMEM((units, nx, count, width), bf16),
            pltpu.VMEM((count, width), f32),
            pltpu.VMEM(w_up.shape, bf16),
            pltpu.VMEM(w_down.shape, bf16),
            pltpu.VMEM((2, count, META), f32),
            pltpu.VMEM((2, count, META), f32),
            pltpu.VMEM((units, nx * count, hid), f32),
            pltpu.VMEM((units, nx * count, hid), f32),
            pltpu.VMEM((units, nx * count, hid), bf16),
            pltpu.VMEM((units, nx, count, width), bf16),
            pltpu.VMEM((units, hops, count, width), bf16),
            pltpu.VMEM((units, hops, count, width), bf16),
            pltpu.VMEM((units, hops, count, width), bf16),
            pltpu.VMEM((units, hops, count, width), bf16),
            pltpu.VMEM((2, units, count, width), bf16),
            pltpu.VMEM((2, units, count, width), bf16),
            dma((4,)),
            dma((2, units)),
            dma((2, units, hops)),
            dma((3, 2, units)),
            dma((3, 2, units, hops)),
            dma((2,)),
            dma((2,)),
            dma((units,)),
            dma((units,)),
        ],
        compiler_params=pltpu.CompilerParams(
            collective_id=0, has_side_effects=True, vmem_limit_bytes=56 * 2**20
        ),
        name="layer",
    )(
        queries,
        key_rows,
        value_rows,
        stream,
        routes,
        seq_length,
        norm_gain.reshape(1, width),
        router,
        w_up,
        w_down,
        (final_gain * value_weight).reshape(1, width),
        value_bias,
    )
    return layer_out, values[:, 0]


def build(mesh, nz, nx, full_width):
    finer = Mesh(
        mesh.devices.reshape(mesh.shape["groups"], nz, nx, mesh.shape["tp"]),
        ("groups", "z", "x", "tp"),
    )
    placed = (
        P(GROUPS_SEQ, "tp"),
        P(GROUPS_SEQ, "tp"),
        P(GROUPS_SEQ, "tp"),
        P(GROUPS_SEQ, "tp"),
        P(GROUPS_SEQ, None),
        P("groups"),
        P("tp"),
        P("tp", None),
        P("tp", SEQ),
        P(SEQ, "tp"),
        P("tp"),
        P("tp"),
        P(),
    )
    return jax.shard_map(
        functools.partial(on_device, (nz, nx, full_width)),
        mesh=finer,
        in_specs=placed,
        out_specs=(P(GROUPS_SEQ, "tp"), P(GROUPS_SEQ)),
        check_vma=False,
    )


def solution(mesh):
    return build(mesh, 16, mesh.shape["seq"] // 16, 6144)
```

```python
import functools
import math

import jax
import jax.numpy as jnp
from jax import lax
from jax.experimental import pallas as pl
from jax.experimental.pallas import tpu as pltpu
from jax.sharding import Mesh
from jax.sharding import PartitionSpec as P

HD = 128
EXPERTS = 4
META = 128
SEQ = ("z", "x")
GROUPS_SEQ = ("groups", "z", "x")
eps = 1e-05
masked = -1e30
f32 = jnp.float32
bf16 = jnp.bfloat16


def lane_sum(a):
    return jnp.sum(a, axis=1, keepdims=True)


def kernel(
    dims,
    queries,
    key_rows,
    value_rows,
    stream,
    routes,
    seq_length,
    norm_gain,
    router,
    w_up_hbm,
    w_down_hbm,
    final_gain,
    value_weight,
    value_bias,
    layer_out,
    values,
    q_all,
    kv_own,
    kv,
    att_out,
    att_in,
    top_score,
    weight_sum,
    mixed_values,
    rows_z,
    rows_x,
    hidden,
    info,
    w_up,
    w_down,
    stats,
    stats_in,
    ups,
    ups_in,
    parts,
    sums,
    recv,
    back_out,
    back_in,
    local_sem,
    asend,
    arecv,
    zsend,
    zrecv,
    xsend,
    xrecv,
    bsend,
    brecv,
    tsend,
    trecv,
    usend,
    urecv,
):
    nz, nx, full_width = dims
    units, hops = nz // 2, nx // 2
    z, x, t = lax.axis_index("z"), lax.axis_index("x"), lax.axis_index("tp")
    right, left = {"x": lax.rem(x + 1, nx)}, {"x": lax.rem(x + nx - 1, nx)}
    twin = {"tp": 1 - t}
    count, width = stream.shape
    kv_width = key_rows.shape[1]
    q_width = width // nx
    sharers = nx // (kv_width // HD)

    def along_z(steps):
        return {"z": lax.rem(z + nz + steps, nz)}

    def remote(src, dst, send, recv, to):
        return pltpu.make_async_remote_copy(
            src_ref=src, dst_ref=dst, send_sem=send, recv_sem=recv, device_id=to,
            device_id_type=pl.DeviceIdType.MESH,
        )

    up_copy = pltpu.make_async_copy(w_up_hbm, w_up, local_sem.at[0])
    down_copy = pltpu.make_async_copy(w_down_hbm, w_down, local_sem.at[1])
    up_copy.start()
    down_copy.start()
    barrier = pltpu.get_barrier_semaphore()

    def greet(peer):
        pl.semaphore_signal(barrier, inc=1, device_id=peer, device_id_type=pl.DeviceIdType.MESH)

    for steps in (1, -1, 2, -2):
        greet(along_z(steps))
    for d in range(1, nx):
        greet({"x": lax.rem(x + d, nx)})
    greet(twin)
    for head in range(kv_width // HD):
        kv_own[head, :, :HD] = key_rows[:, head * HD : (head + 1) * HD]
        kv_own[head, :, HD:] = value_rows[:, head * HD : (head + 1) * HD]
    kv[0, 0, x] = kv_own[x // sharers]
    q_all[x] = queries[:, pl.ds(pl.multiple_of(x * q_width, HD), q_width)]
    pl.semaphore_wait(barrier, 4 + nx)

    def q_copy(d):
        peer = lax.rem(x + d, nx)
        at = pl.ds(pl.multiple_of(peer * q_width, HD), q_width)
        return remote(queries.at[:, at], q_all.at[x], asend.at[0, d], arecv.at[0, d], {"x": peer})

    def kv_copy(d):
        peer = lax.rem(x + d, nx)
        return remote(kv_own.at[peer // sharers], kv.at[0, 0, x], asend.at[1, d], arecv.at[1, d], {"x": peer})

    def att_copy(d):
        peer = lax.rem(x + d, nx)
        return remote(att_out.at[peer], att_in.at[x], asend.at[2, d], arecv.at[2, d], {"x": peer})

    far_first = sorted(range(1, nx), key=lambda d: -min(d, nx - d))
    for d in far_first:
        kv_copy(d).start()
    for d in far_first:
        q_copy(d).start()

    def z_ring(phase, at):
        def first(way, u):
            steps = (-u if u < 3 else -2) if way == 0 else min(u + 1, 2)
            src = at(0, 0) if (u < 3 and way == 0) or u < 2 else at(u - 2, way)
            return remote(src, at(u, way), zsend.at[way, u], zrecv.at[phase, way, u], along_z(steps))

        def onward(way, u):
            return remote(
                at(u - 2, way), at(u, way), zsend.at[way, u], zrecv.at[phase, way, u],
                along_z(-2 if way == 0 else 2),
            )

        def start():
            for way, u in ((0, 2), (1, 1), (0, 1), (1, 0)):
                first(way, u).start()

        def take(u):
            @pl.when(u > 0)
            def _():
                onward(0, u).wait_recv()

                @pl.when(u + 2 < units)
                def _():
                    onward(0, u + 2).start()

            onward(1, u).wait_recv()

            @pl.when(u + 2 < units)
            def _():
                onward(1, u + 2).start()

        def drain(u):
            @pl.when(u > 0)
            def _():
                onward(0, u).wait_send()

            onward(1, u).wait_send()

        return start, take, drain

    kv_start, kv_take, kv_drain = z_ring(0, lambda u, half: kv.at[lax.max(u, 0), half])
    for d in range(1, nx):
        kv_copy(d).wait_recv()
    kv_start()
    for d in range(1, nx):
        q_copy(d).wait_recv()

    mine = nx * count
    per = q_width // HD
    limit = seq_length[0]
    top_score[...] = jnp.full(top_score.shape, masked, f32)
    weight_sum[...] = jnp.zeros(weight_sum.shape, f32)
    mixed_values[...] = jnp.zeros(mixed_values.shape, f32)
    q_row = lax.broadcasted_iota(jnp.int32, (per * mine, 2 * mine), 0)
    k_row = lax.broadcasted_iota(jnp.int32, (per * mine, 2 * mine), 1)
    q_pos = z * mine + lax.rem(q_row, mine)

    def attend(u, carry):
        kv_take(u)
        q = jnp.concatenate(
            [q_all[:, :, j * HD : (j + 1) * HD].reshape(mine, HD) for j in range(per)], axis=0
        )
        k = kv[u, :, :, :, :HD].reshape(2 * mine, HD)
        v = kv[u, :, :, :, HD:].reshape(2 * mine, HD)
        s = lax.dot_general(q, k, (((1,), (1,)), ((), ())), preferred_element_type=f32) * (1.0 / math.sqrt(HD))
        k_pos = jnp.where(
            k_row < mine, lax.rem(z + u, nz) * mine + k_row, lax.rem(z - u - 1 + nz, nz) * mine + k_row - mine
        )
        allowed = (k_pos <= q_pos) & (k_pos < limit)
        s = jnp.where(allowed, s, masked)
        old = top_score[:, 0:1]
        new = jnp.maximum(old, jnp.max(s, axis=1, keepdims=True))
        p = jnp.where(allowed, jnp.exp(s - new), 0.0)
        keep = jnp.exp(old - new)
        top_score[...] = jnp.broadcast_to(new, top_score.shape)
        weight_sum[...] = weight_sum[...] * keep + lane_sum(p)
        mixed_values[...] = mixed_values[...] * keep + jnp.dot(p.astype(bf16), v, preferred_element_type=f32)
        return carry

    lax.fori_loop(0, units, attend, 0)
    attended = mixed_values[...] / weight_sum[...]
    for s in range(nx):
        for j in range(per):
            piece = attended[j * mine + s * count : j * mine + (s + 1) * count]
            att_out[s, :, j * HD : (j + 1) * HD] = piece.astype(bf16)
    att_in[x] = att_out[x]
    for d in far_first:
        att_copy(d).start()
    for d in range(1, nz):
        greet(along_z(d))

    def kv_sent(u, carry):
        kv_drain(u)
        return carry

    lax.fori_loop(0, units, kv_sent, 0)
    for d in range(1, nx):
        kv_copy(d).wait_send()
        q_copy(d).wait_send()
    for d in range(1, nx):
        att_copy(d).wait_recv()
    for s in range(nx):
        at = slice(s * q_width, (s + 1) * q_width)
        hidden[:, at] = stream[:, at].astype(f32) + att_in[s].astype(f32)

    def both(index, message):
        stats[index] = message
        copy = remote(stats.at[index], stats_in.at[index], tsend.at[index], trecv.at[index], twin)
        copy.start()
        copy.wait()
        return message + stats_in[index]

    lane = lax.broadcasted_iota(jnp.int32, (count, META), 1)
    row = lax.broadcasted_iota(jnp.int32, (count, META), 0)

    def upright(line):
        return lane_sum(jnp.where(lane == row, jnp.broadcast_to(line, (count, META)), 0.0))

    h_all = hidden[...]
    gained = h_all * norm_gain[...]
    message = jnp.where(lane == EXPERTS, lane_sum(h_all * h_all), 0.0)
    for e in range(EXPERTS):
        message = jnp.where(lane == e, lane_sum(gained * router[e : e + 1]), message)
    total = both(0, message)
    sq = lane_sum(jnp.where(lane == EXPERTS, total, 0.0))
    scale = lax.rsqrt(sq / full_width + eps)
    logits = total * scale
    spread = jnp.concatenate([routes[...].astype(f32), jnp.zeros((2, META - count), f32)], axis=1)
    first, second = upright(spread[0:1]).astype(jnp.int32), upright(spread[1:2]).astype(jnp.int32)
    hit_a, hit_b = lane == first, lane == second
    gap = lane_sum(jnp.where(hit_a, logits, 0.0)) - lane_sum(jnp.where(hit_b, logits, 0.0))
    gate_a, gate_b = 1.0 / (1.0 + jnp.exp(-gap)), 1.0 / (1.0 + jnp.exp(gap))
    hits = jnp.where(hit_a | hit_b, 1.0, 0.0)
    rank = jnp.zeros((count, META), f32)
    for i in range(count - 1):
        rank = rank + jnp.where(row > i, jnp.broadcast_to(hits[i : i + 1], (count, META)), 0.0)
    place = jnp.where(hits > 0.5, rank + 1.0, 0.0)
    rows_z[0, 0, :, :width] = (gained * scale).astype(bf16)
    rows_z[0, 0, :, width:] = place.astype(bf16)
    rows_start, rows_take, rows_drain = z_ring(1, lambda u, half: rows_z.at[lax.max(u, 0), half])
    rows_start()
    info[0] = place
    info[1] = jnp.where(hit_a, gate_a, jnp.where(hit_b, gate_b, 0.0))

    my_expert = z // (nz // EXPERTS)
    slots = count // 2

    def column(table, expert):
        return lane_sum(jnp.where(lane == expert, table, 0.0))

    def choose(u):
        out = jnp.zeros((count, width), f32)
        for half in (0, 1):
            block = rows_z[u, half].astype(f32)
            places = jnp.broadcast_to(column(block[:, width:], my_expert), (count, META))
            for i in range(count):
                want = jnp.broadcast_to(places[i : i + 1], (count, META)) + (slots * half)
                chosen = jnp.where(((row + 1).astype(f32) == want) & (want > slots * half + 0.5), 1.0, 0.0)
                out = out + chosen[:, 0:1] * block[i : i + 1, :width]
        rows_x[u, x] = out.astype(bf16)

    def g_copy(way, u, h):
        back = nx - (h - 1) if way == 0 else h - 1
        at = rows_x.at[u, lax.rem(x + back, nx)]
        return remote(
            at, at, xsend.at[0, way, u, h - 1], xrecv.at[0, way, u, h - 1], right if way == 0 else left
        )

    def ups_copy(u):
        return remote(ups.at[u], ups_in.at[u], usend.at[u], urecv.at[u], twin)

    def project(u):
        ups[u] = jnp.dot(rows_x[u].reshape(mine, width), w_up[...], preferred_element_type=f32)
        ups_copy(u).start()

    def own(way, u, k):
        ahead = hops - k
        return parts.at[u, lax.rem(x + (ahead if way == 0 else nx - ahead), nx)]

    def r_copy(way, u, k, src):
        return remote(
            src, recv.at[way, u, k], xsend.at[1, way, u, k], xrecv.at[1, way, u, k], right if way == 0 else left
        )

    def expand(u):
        ups_copy(u).wait_recv()
        v = ups[u] + ups_in[u]
        active = (v / (1.0 + jnp.exp(-v))).astype(bf16)
        made = jnp.dot(active, w_down[...], preferred_element_type=f32)
        for d in range(nx):
            parts[u, d] = made[d * count : (d + 1) * count].astype(bf16)
        for way in (0, 1):

            @pl.when(lax.rem(u, 2) == way)
            def _():
                r_copy(way, u, 0, own(way, u, 0)).start()

    def back_copy(half, u):
        steps = u if half == 0 else -u - 1
        return remote(back_out.at[u, half], back_in.at[u, half], bsend.at[half, u], brecv.at[half, u], along_z(steps))

    def home(u):
        for way in (0, 1):
            r_copy(way, u, hops - 1, own(way, u, hops - 1)).wait_recv()
        both_ways = recv[0, u, hops - 1].astype(f32) + recv[1, u, hops - 1].astype(f32)
        done = (parts[u, x].astype(f32) + both_ways).astype(bf16)

        @pl.when(u > 0)
        def _():
            back_out[u, 0] = done[:slots]
            back_copy(0, u).start()

        @pl.when(u == 0)
        def _():
            back_in[0, 0] = done[:slots]

        back_out[u, 1] = done[slots:]
        back_copy(1, u).start()

    def blend(u):
        @pl.when(u > 0)
        def _():
            back_copy(0, u).wait_recv()

        back_copy(1, u).wait_recv()
        mix = hidden[...]
        for half in (0, 1):
            source = lax.rem(z - u + nz, nz) if half == 0 else lax.rem(z + u + 1, nz)
            expert = source // (nz // EXPERTS)
            places, gate = column(info[0], expert), column(info[1], expert)
            got = back_in[u, half].astype(f32)
            for i in range(slots):
                mix = mix + jnp.where(places == float(i + 1), gate, 0.0) * got[i : i + 1]
        hidden[...] = mix

    for d in range(1, nx):
        att_copy(d).wait_send()
    up_copy.wait()
    down_copy.wait()
    pl.semaphore_wait(barrier, nz - 1)
    lag = hops + 1

    def slot(step, carry):
        @pl.when(step < units)
        def _():
            rows_take(step)
            choose(step)
            g_copy(0, step, 1).start()
            g_copy(1, step, 1).start()

        for h in range(1, hops):
            u = step - h

            @pl.when((u >= 0) & (u < units))
            def _():
                for way in (0, 1):
                    g_copy(way, u, h).wait_recv()
                    if h < hops - 1:
                        g_copy(way, u, h + 1).start()
                    else:

                        @pl.when(lax.rem(u, 2) == way)
                        def _():
                            g_copy(way, u, h + 1).start()

        for k in range(1, hops):
            u = step - lag - k

            @pl.when((u >= 0) & (u < units))
            def _():
                for way in (0, 1):

                    def add():
                        r_copy(way, u, k - 1, own(way, u, k - 1)).wait_recv()
                        total = recv[way, u, k - 1].astype(f32) + own(way, u, k)[...].astype(f32)
                        sums[way, u, k] = total.astype(bf16)
                        r_copy(way, u, k, sums.at[way, u, k]).start()

                    if k > 1:
                        add()
                    else:
                        pl.when(lax.rem(u, 2) == way)(add)

                        @pl.when(lax.rem(u, 2) != way)
                        def _():
                            r_copy(way, u, k, own(way, u, k)).start()

        u_in = step - hops

        @pl.when((u_in >= 0) & (u_in < units))
        def _():
            for way in (0, 1):

                @pl.when(lax.rem(u_in, 2) == way)
                def _():
                    g_copy(way, u_in, hops).wait_recv()

            project(u_in)

        u_mid = step - lag

        @pl.when((u_mid >= 0) & (u_mid < units))
        def _():
            expand(u_mid)

        u_out = step - lag - hops

        @pl.when((u_out >= 0) & (u_out < units))
        def _():
            home(u_out)

        u_last = step - lag - hops - 2

        @pl.when(u_last >= 0)
        def _():
            blend(u_last)

        return carry

    lax.fori_loop(0, units + lag + hops + 2, slot, 0)
    out = hidden[...]
    layer_out[...] = out.astype(bf16)
    message = jnp.where(lane == 0, lane_sum(out * out), 0.0)
    message = jnp.where(lane == 1, lane_sum(out * (final_gain[...] * value_weight[...])), message)
    total = both(1, message)
    estimate = total[:, 1:2] * lax.rsqrt(total[:, 0:1] / full_width + eps) + value_bias[0]
    real = (z * nx + x) * count + row < limit
    flat = jnp.sum(jnp.where((lane == row) & real, estimate, 0.0), axis=0, keepdims=True)
    values[...] = flat

    def drain(u, carry):
        rows_drain(u)
        ups_copy(u).wait_send()

        @pl.when(u > 0)
        def _():
            back_copy(0, u).wait_send()

        back_copy(1, u).wait_send()
        for way in (0, 1):
            for k in range(1, hops):
                g_copy(way, u, k).wait_send()
                r_copy(way, u, k, own(way, u, k)).wait_send()

            @pl.when(lax.rem(u, 2) == way)
            def _():
                g_copy(way, u, hops).wait_send()
                r_copy(way, u, 0, own(way, u, 0)).wait_send()

        return carry

    lax.fori_loop(0, units, drain, 0)


def on_device(dims, *args):
    (stream, queries, key_rows, value_rows, routes, seq_length, norm_gain, router) = args[:8]
    (w_up, w_down, final_gain, value_weight, value_bias) = args[8:]
    nz, nx, _ = dims
    units, hops = nz // 2, nx // 2
    count, width = stream.shape
    hid = w_up.shape[1]
    heads = key_rows.shape[1] // HD
    mine = nx * count
    stacked = width // nx // HD * mine
    vmem, smem, far = (
        pl.BlockSpec(memory_space=pltpu.VMEM),
        pl.BlockSpec(memory_space=pltpu.SMEM),
        pl.BlockSpec(memory_space=pl.ANY),
    )
    dma = pltpu.SemaphoreType.DMA
    layer_out, values = pl.pallas_call(
        functools.partial(kernel, dims),
        out_shape=(
            jax.ShapeDtypeStruct((count, width), bf16),
            jax.ShapeDtypeStruct((1, META), f32),
        ),
        in_specs=[vmem, vmem, vmem, vmem, vmem, smem, vmem, vmem, far, far, vmem, vmem, smem],
        out_specs=(vmem, vmem),
        scratch_shapes=[
            pltpu.VMEM((nx, count, width // nx), bf16),
            pltpu.VMEM((heads, count, 2 * HD), bf16),
            pltpu.VMEM((units, 2, nx, count, 2 * HD), bf16),
            pltpu.VMEM((nx, count, width // nx), bf16),
            pltpu.VMEM((nx, count, width // nx), bf16),
            pltpu.VMEM((stacked, HD), f32),
            pltpu.VMEM((stacked, HD), f32),
            pltpu.VMEM((stacked, HD), f32),
            pltpu.VMEM((units, 2, count, width + META), bf16),
            pltpu.VMEM((units, nx, count, width), bf16),
            pltpu.VMEM((count, width), f32),
            pltpu.VMEM((2, count, META), f32),
            pltpu.VMEM(w_up.shape, bf16),
            pltpu.VMEM(w_down.shape, bf16),
            pltpu.VMEM((2, count, META), f32),
            pltpu.VMEM((2, count, META), f32),
            pltpu.VMEM((units, mine, hid), f32),
            pltpu.VMEM((units, mine, hid), f32),
            pltpu.VMEM((units, nx, count, width), bf16),
            pltpu.VMEM((2, units, hops, count, width), bf16),
            pltpu.VMEM((2, units, hops, count, width), bf16),
            pltpu.VMEM((units, 2, count // 2, width), bf16),
            pltpu.VMEM((units, 2, count // 2, width), bf16),
            dma((2,)),
            dma((3, nx)),
            dma((3, nx)),
            dma((2, units)),
            dma((2, 2, units)),
            dma((2, 2, units, hops)),
            dma((2, 2, units, hops)),
            dma((2, units)),
            dma((2, units)),
            dma((2,)),
            dma((2,)),
            dma((units,)),
            dma((units,)),
        ],
        compiler_params=pltpu.CompilerParams(
            collective_id=0, has_side_effects=True, vmem_limit_bytes=56 * 2**20
        ),
        name="layer",
    )(
        queries,
        key_rows,
        value_rows,
        stream,
        routes.T,
        seq_length,
        norm_gain.reshape(1, width),
        router.T,
        w_up,
        w_down,
        final_gain.reshape(1, width),
        value_weight.reshape(1, width),
        value_bias,
    )
    return layer_out, values[0, :count]


def build(mesh, nz, nx, full_width):
    finer = Mesh(
        mesh.devices.reshape(mesh.shape["groups"], nz, nx, mesh.shape["tp"]),
        ("groups", "z", "x", "tp"),
    )
    placed = (
        P(GROUPS_SEQ, "tp"),
        P(GROUPS_SEQ, "tp"),
        P(GROUPS_SEQ, "tp"),
        P(GROUPS_SEQ, "tp"),
        P(GROUPS_SEQ, None),
        P("groups"),
        P("tp"),
        P("tp", None),
        P("tp", SEQ),
        P(SEQ, "tp"),
        P("tp"),
        P("tp"),
        P(),
    )
    return jax.shard_map(
        functools.partial(on_device, (nz, nx, full_width)),
        mesh=finer,
        in_specs=placed,
        out_specs=(P(GROUPS_SEQ, "tp"), P(GROUPS_SEQ)),
        check_vma=False,
    )


def solution(mesh):
    return build(mesh, 16, mesh.shape["seq"] // 16, 6144)
```

```python
import functools
import math

import jax
import jax.numpy as jnp
from jax import lax
from jax.experimental import pallas as pl
from jax.experimental.pallas import tpu as pltpu
from jax.sharding import Mesh
from jax.sharding import PartitionSpec as P

HD = 128
EXPERTS = 4
META = 128
SEQ = ("z", "x")
GROUPS_SEQ = ("groups", "z", "x")
eps = 1e-05
masked = -1e30
chunks = 4
f32 = jnp.float32
bf16 = jnp.bfloat16


def lane_sum(a):
    return jnp.sum(a, axis=1, keepdims=True)


def kernel(
    dims,
    queries,
    key_rows,
    value_rows,
    stream,
    routes,
    seq_length,
    norm_gain,
    router,
    w_up_hbm,
    w_down_hbm,
    final_gain,
    value_weight,
    value_bias,
    layer_out,
    values,
    q_all,
    kv_own,
    kv,
    att_out,
    att_in,
    top_score,
    weight_sum,
    mixed_values,
    rows_out,
    rows_z,
    rows_x,
    hidden,
    info,
    w_up,
    w_down,
    w_up_in,
    w_down_in,
    stats,
    stats_in,
    ups,
    ups_out,
    ups_in,
    ups_half,
    ups_twin,
    act_out,
    act_in,
    parts,
    sums,
    recv,
    back_out,
    back_in,
    local_sem,
    asend,
    arecv,
    zsend,
    zrecv,
    xsend,
    xrecv,
    bsend,
    brecv,
    tsend,
    trecv,
    usend,
    urecv,
    wsend,
    wrecv,
):
    nz, nx, full_width = dims
    units, hops = nz // 2, nx // 2
    z, x, t = lax.axis_index("z"), lax.axis_index("x"), lax.axis_index("tp")
    right, left = {"x": lax.rem(x + 1, nx)}, {"x": lax.rem(x + nx - 1, nx)}
    twin = {"tp": 1 - t}
    count, width = stream.shape
    kv_width = key_rows.shape[1]
    q_width = width // nx
    sharers = nx // (kv_width // HD)

    def along_z(steps):
        return {"z": lax.rem(z + nz + steps, nz)}

    def remote(src, dst, send, recv, to):
        return pltpu.make_async_remote_copy(
            src_ref=src, dst_ref=dst, send_sem=send, recv_sem=recv, device_id=to,
            device_id_type=pl.DeviceIdType.MESH,
        )

    c = lax.rem(z, 2)
    m, pairs = z // 2, nz // 2
    narrow, hid = width // 2, w_up_hbm.shape[1]
    mate = {"z": z + 1 - 2 * c}
    keep_cols = pl.ds(pl.multiple_of(c * narrow, HD), narrow)
    give_cols = pl.ds(pl.multiple_of((1 - c) * narrow, HD), narrow)
    up_copy = pltpu.make_async_copy(w_up_hbm.at[keep_cols, :], w_up, local_sem.at[0])
    down_copy = pltpu.make_async_copy(w_down_hbm.at[:, keep_cols], w_down, local_sem.at[1])

    def weight_copy(k):
        if k < chunks:
            size = narrow // chunks
            at = pl.ds(pl.multiple_of((1 - c) * narrow + k * size, HD // 2), size)
            return remote(
                w_up_hbm.at[at, :], w_up_in.at[pl.ds(k * size, size), :], wsend.at[k], wrecv.at[k], mate
            )
        size = hid // chunks
        at = pl.ds((k - chunks) * size, size)
        return remote(w_down_hbm.at[at, give_cols], w_down_in.at[at, :], wsend.at[k], wrecv.at[k], mate)

    up_copy.start()
    down_copy.start()
    barrier = pltpu.get_barrier_semaphore()

    def greet(peer):
        pl.semaphore_signal(barrier, inc=1, device_id=peer, device_id_type=pl.DeviceIdType.MESH)

    for steps in (1, -1, 2, -2):
        greet(along_z(steps))
    for d in range(1, nx):
        greet({"x": lax.rem(x + d, nx)})
    greet(twin)
    for head in range(kv_width // HD):
        kv_own[head, :, :HD] = key_rows[:, head * HD : (head + 1) * HD]
        kv_own[head, :, HD:] = value_rows[:, head * HD : (head + 1) * HD]
    kv[0, 0, x] = kv_own[x // sharers]
    q_all[x] = queries[:, pl.ds(pl.multiple_of(x * q_width, HD), q_width)]
    pl.semaphore_wait(barrier, 4 + nx)

    def q_copy(d):
        peer = lax.rem(x + d, nx)
        at = pl.ds(pl.multiple_of(peer * q_width, HD), q_width)
        return remote(queries.at[:, at], q_all.at[x], asend.at[0, d], arecv.at[0, d], {"x": peer})

    def kv_copy(d):
        peer = lax.rem(x + d, nx)
        return remote(kv_own.at[peer // sharers], kv.at[0, 0, x], asend.at[1, d], arecv.at[1, d], {"x": peer})

    def att_copy(d):
        peer = lax.rem(x + d, nx)
        return remote(att_out.at[peer], att_in.at[x], asend.at[2, d], arecv.at[2, d], {"x": peer})

    far_first = sorted(range(1, nx), key=lambda d: -min(d, nx - d))
    for d in far_first:
        kv_copy(d).start()
    for d in far_first:
        q_copy(d).start()

    def z_ring(phase, at):
        def first(way, u):
            steps = (-u if u < 3 else -2) if way == 0 else min(u + 1, 2)
            src = at(0, 0) if (u < 3 and way == 0) or u < 2 else at(u - 2, way)
            return remote(src, at(u, way), zsend.at[way, u], zrecv.at[phase, way, u], along_z(steps))

        def onward(way, u):
            return remote(
                at(u - 2, way), at(u, way), zsend.at[way, u], zrecv.at[phase, way, u],
                along_z(-2 if way == 0 else 2),
            )

        def start():
            for way, u in ((0, 2), (1, 1), (0, 1), (1, 0)):
                first(way, u).start()

        def take(u):
            @pl.when(u > 0)
            def _():
                onward(0, u).wait_recv()

                @pl.when(u + 2 < units)
                def _():
                    onward(0, u + 2).start()

            onward(1, u).wait_recv()

            @pl.when(u + 2 < units)
            def _():
                onward(1, u + 2).start()

        def drain(u):
            @pl.when(u > 0)
            def _():
                onward(0, u).wait_send()

            onward(1, u).wait_send()

        return start, take, drain

    kv_start, kv_take, kv_drain = z_ring(0, lambda u, half: kv.at[lax.max(u, 0), half])
    for d in range(1, nx):
        kv_copy(d).wait_recv()
    kv_start()
    for d in range(1, nx):
        q_copy(d).wait_recv()

    mine = nx * count
    per = q_width // HD
    limit = seq_length[0]
    top_score[...] = jnp.full(top_score.shape, masked, f32)
    weight_sum[...] = jnp.zeros(weight_sum.shape, f32)
    mixed_values[...] = jnp.zeros(mixed_values.shape, f32)
    q_row = lax.broadcasted_iota(jnp.int32, (per * mine, 2 * mine), 0)
    k_row = lax.broadcasted_iota(jnp.int32, (per * mine, 2 * mine), 1)
    q_pos = z * mine + lax.rem(q_row, mine)

    def attend(u, carry):
        kv_take(u)
        q = jnp.concatenate(
            [q_all[:, :, j * HD : (j + 1) * HD].reshape(mine, HD) for j in range(per)], axis=0
        )
        k = kv[u, :, :, :, :HD].reshape(2 * mine, HD)
        v = kv[u, :, :, :, HD:].reshape(2 * mine, HD)
        s = lax.dot_general(q, k, (((1,), (1,)), ((), ())), preferred_element_type=f32) * (1.0 / math.sqrt(HD))
        k_pos = jnp.where(
            k_row < mine, lax.rem(z + u, nz) * mine + k_row, lax.rem(z - u - 1 + nz, nz) * mine + k_row - mine
        )
        allowed = (k_pos <= q_pos) & (k_pos < limit)
        s = jnp.where(allowed, s, masked)
        old = top_score[:, 0:1]
        new = jnp.maximum(old, jnp.max(s, axis=1, keepdims=True))
        p = jnp.where(allowed, jnp.exp(s - new), 0.0)
        keep = jnp.exp(old - new)
        top_score[...] = jnp.broadcast_to(new, top_score.shape)
        weight_sum[...] = weight_sum[...] * keep + lane_sum(p)
        mixed_values[...] = mixed_values[...] * keep + jnp.dot(p.astype(bf16), v, preferred_element_type=f32)
        return carry

    each = 2 * chunks // units
    for u in range(units):
        attend(u, 0)
        for k in range(u * each, (u + 1) * each):
            weight_copy(k).start()
    attended = mixed_values[...] / weight_sum[...]
    for s in range(nx):
        for j in range(per):
            piece = attended[j * mine + s * count : j * mine + (s + 1) * count]
            att_out[s, :, j * HD : (j + 1) * HD] = piece.astype(bf16)
    att_in[x] = att_out[x]
    for d in far_first:
        att_copy(d).start()
    for d in range(1, nz):
        greet(along_z(d))

    def kv_sent(u, carry):
        kv_drain(u)
        return carry

    lax.fori_loop(0, units, kv_sent, 0)
    for d in range(1, nx):
        kv_copy(d).wait_send()
        q_copy(d).wait_send()
    for d in range(1, nx):
        att_copy(d).wait_recv()
    for s in range(nx):
        at = slice(s * q_width, (s + 1) * q_width)
        hidden[:, at] = stream[:, at].astype(f32) + att_in[s].astype(f32)

    def both(index, message):
        stats[index] = message
        copy = remote(stats.at[index], stats_in.at[index], tsend.at[index], trecv.at[index], twin)
        copy.start()
        copy.wait()
        return message + stats_in[index]

    lane = lax.broadcasted_iota(jnp.int32, (count, META), 1)
    row = lax.broadcasted_iota(jnp.int32, (count, META), 0)

    def upright(line):
        return lane_sum(jnp.where(lane == row, jnp.broadcast_to(line, (count, META)), 0.0))

    h_all = hidden[...]
    gained = h_all * norm_gain[...]
    message = jnp.where(lane == EXPERTS, lane_sum(h_all * h_all), 0.0)
    for e in range(EXPERTS):
        message = jnp.where(lane == e, lane_sum(gained * router[e : e + 1]), message)
    total = both(0, message)
    sq = lane_sum(jnp.where(lane == EXPERTS, total, 0.0))
    scale = lax.rsqrt(sq / full_width + eps)
    logits = total * scale
    spread = jnp.concatenate([routes[...].astype(f32), jnp.zeros((2, META - count), f32)], axis=1)
    first, second = upright(spread[0:1]).astype(jnp.int32), upright(spread[1:2]).astype(jnp.int32)
    hit_a, hit_b = lane == first, lane == second
    gap = lane_sum(jnp.where(hit_a, logits, 0.0)) - lane_sum(jnp.where(hit_b, logits, 0.0))
    gate_a, gate_b = 1.0 / (1.0 + jnp.exp(-gap)), 1.0 / (1.0 + jnp.exp(gap))
    hits = jnp.where(hit_a | hit_b, 1.0, 0.0)
    rank = jnp.zeros((count, META), f32)
    for i in range(count - 1):
        rank = rank + jnp.where(row > i, jnp.broadcast_to(hits[i : i + 1], (count, META)), 0.0)
    place = jnp.where(hits > 0.5, rank + 1.0, 0.0)
    normed = gained * scale
    low, high = normed[:, :narrow], normed[:, narrow:]
    rows_out[:, :narrow] = jnp.where(c == 0, high, low).astype(bf16)
    rows_out[:, narrow:] = place.astype(bf16)
    rows_z[0, c, :, :narrow] = jnp.where(c == 0, low, high).astype(bf16)
    rows_z[0, c, :, narrow:] = place.astype(bf16)

    def mate_rows():
        return remote(rows_out, rows_z.at[0, c], zsend.at[0, 0], zrecv.at[1, 0, 0], mate)

    def rows_copy(b, u):
        return remote(
            rows_z.at[lax.max(u - 2, 0), b], rows_z.at[u, b], zsend.at[b, u], zrecv.at[1, b, u],
            along_z(2 - 4 * lax.rem(u, 2)),
        )

    mate_rows().start()

    def rows_take(u):
        @pl.when(u == 0)
        def _():
            mate_rows().wait_recv()
            for b in (0, 1):
                rows_copy(b, 1).start()
                rows_copy(b, 2).start()

        @pl.when(u > 0)
        def _():
            for b in (0, 1):
                rows_copy(b, u).wait_recv()

                @pl.when(u + 2 < units)
                def _():
                    rows_copy(b, u + 2).start()

    def rows_drain(u):
        @pl.when(u == 0)
        def _():
            mate_rows().wait_send()

        @pl.when(u > 0)
        def _():
            for b in (0, 1):
                rows_copy(b, u).wait_send()

    info[0] = place
    info[1] = jnp.where(hit_a, gate_a, jnp.where(hit_b, gate_b, 0.0))

    my_expert = z // (nz // EXPERTS)
    slots = count // 2

    def column(table, expert):
        return lane_sum(jnp.where(lane == expert, table, 0.0))

    def choose(u):
        out = jnp.zeros((count, narrow), f32)
        for half in (0, 1):
            block = rows_z[u, half].astype(f32)
            places = jnp.broadcast_to(column(block[:, narrow:], my_expert), (count, META))
            for i in range(count):
                want = jnp.broadcast_to(places[i : i + 1], (count, META)) + (slots * half)
                chosen = jnp.where(((row + 1).astype(f32) == want) & (want > slots * half + 0.5), 1.0, 0.0)
                out = out + chosen[:, 0:1] * block[i : i + 1, :narrow]
        rows_x[u, x] = out.astype(bf16)

    def g_copy(way, u, h):
        back = nx - (h - 1) if way == 0 else h - 1
        at = rows_x.at[u, lax.rem(x + back, nx)]
        return remote(
            at, at, xsend.at[0, way, u, h - 1], xrecv.at[0, way, u, h - 1], right if way == 0 else left
        )

    def ups_copy(u):
        return remote(ups_out.at[u], ups_in.at[u], usend.at[0, u], urecv.at[0, u], mate)

    def twin_copy(u):
        return remote(ups_half.at[u], ups_twin.at[u], usend.at[1, u], urecv.at[1, u], twin)

    def act_copy(u):
        return remote(act_out.at[u], act_in.at[u], usend.at[2, u], urecv.at[2, u], mate)

    def project(u):
        got = rows_x[u].reshape(mine, narrow)
        ups_out[u] = jnp.dot(got, w_up_in[...], preferred_element_type=f32).astype(bf16)
        ups_copy(u).start()
        ups[u] = jnp.dot(got, w_up[...], preferred_element_type=f32)

    def merge(u):
        ups_copy(u).wait_recv()
        ups_half[u] = ups[u] + ups_in[u].astype(f32)
        twin_copy(u).start()

    def activate(u):
        twin_copy(u).wait_recv()
        v = ups_half[u] + ups_twin[u]
        act_out[u] = (v / (1.0 + jnp.exp(-v))).astype(bf16)
        act_copy(u).start()

    def own(way, u, k):
        ahead = hops - k
        return parts.at[u, lax.rem(x + (ahead if way == 0 else nx - ahead), nx)]

    def r_copy(way, u, k, src):
        return remote(
            src, recv.at[way, u, k], xsend.at[1, way, u, k], xrecv.at[1, way, u, k], right if way == 0 else left
        )

    def expand(u):
        act_copy(u).wait_recv()
        made = jnp.dot(act_out[u], w_down[...], preferred_element_type=f32)
        made = made + jnp.dot(act_in[u], w_down_in[...], preferred_element_type=f32)
        for d in range(nx):
            parts[u, d] = made[d * count : (d + 1) * count].astype(bf16)
        for way in (0, 1):

            @pl.when(lax.rem(u, 2) == way)
            def _():
                r_copy(way, u, 0, own(way, u, 0)).start()

    def offset(u):
        return ((u + 1) // 2) * (2 * lax.rem(u, 2) - 1)

    def back_copy(b, u):
        to = {"z": 2 * lax.rem(m + offset(u) + pairs, pairs) + b}
        return remote(back_out.at[u, b], back_in.at[u, c], bsend.at[b, u], brecv.at[c, u], to)

    def back_arrival(b, u):
        to = {"z": 2 * lax.rem(m + offset(u) + pairs, pairs) + b}
        return remote(back_out.at[u, b], back_in.at[u, b], bsend.at[b, u], brecv.at[b, u], to)

    def home(u):
        for way in (0, 1):
            r_copy(way, u, hops - 1, own(way, u, hops - 1)).wait_recv()
        both_ways = recv[0, u, hops - 1].astype(f32) + recv[1, u, hops - 1].astype(f32)
        done = (parts[u, x].astype(f32) + both_ways).astype(bf16)

        for b in (0, 1):
            back_out[u, b] = done[b * slots : (b + 1) * slots]

            @pl.when((u > 0) | (c != b))
            def _():
                back_copy(b, u).start()

            @pl.when((u == 0) & (c == b))
            def _():
                back_in[0, b] = done[b * slots : (b + 1) * slots]

    def blend(u):
        source = lax.rem(m - offset(u) + pairs, pairs)
        expert = 2 * source // (nz // EXPERTS)
        places, gate = column(info[0], expert), column(info[1], expert)
        weights = [jnp.where(places == float(i + 1), gate, 0.0) for i in range(slots)]
        for b in (0, 1):

            @pl.when((u > 0) | (c != b))
            def _():
                back_arrival(b, u).wait_recv()

            at = slice(b * narrow, (b + 1) * narrow)
            got = back_in[u, b].astype(f32)
            mix = hidden[:, at]
            for i in range(slots):
                mix = mix + weights[i] * got[i : i + 1]
            hidden[:, at] = mix

    for d in range(1, nx):
        att_copy(d).wait_send()
    up_copy.wait()
    down_copy.wait()
    pl.semaphore_wait(barrier, nz - 1)
    for k in range(2 * chunks):
        weight_copy(k).wait_recv()
    lag = hops + 3

    def slot(step, carry):
        @pl.when(step < units)
        def _():
            rows_take(step)
            choose(step)
            g_copy(0, step, 1).start()
            g_copy(1, step, 1).start()

        for h in range(1, hops):
            u = step - h

            @pl.when((u >= 0) & (u < units))
            def _():
                for way in (0, 1):
                    g_copy(way, u, h).wait_recv()
                    if h < hops - 1:
                        g_copy(way, u, h + 1).start()
                    else:

                        @pl.when(lax.rem(u, 2) == way)
                        def _():
                            g_copy(way, u, h + 1).start()

        for k in range(1, hops):
            u = step - lag - k

            @pl.when((u >= 0) & (u < units))
            def _():
                for way in (0, 1):

                    def add():
                        r_copy(way, u, k - 1, own(way, u, k - 1)).wait_recv()
                        total = recv[way, u, k - 1].astype(f32) + own(way, u, k)[...].astype(f32)
                        sums[way, u, k] = total.astype(bf16)
                        r_copy(way, u, k, sums.at[way, u, k]).start()

                    if k > 1:
                        add()
                    else:
                        pl.when(lax.rem(u, 2) == way)(add)

                        @pl.when(lax.rem(u, 2) != way)
                        def _():
                            r_copy(way, u, k, own(way, u, k)).start()

        u_in = step - hops

        @pl.when((u_in >= 0) & (u_in < units))
        def _():
            for way in (0, 1):

                @pl.when(lax.rem(u_in, 2) == way)
                def _():
                    g_copy(way, u_in, hops).wait_recv()

            project(u_in)

        for later, work in ((1, merge), (2, activate)):
            u_next = step - hops - later
            pl.when((u_next >= 0) & (u_next < units))(functools.partial(work, u_next))

        u_mid = step - lag

        @pl.when((u_mid >= 0) & (u_mid < units))
        def _():
            expand(u_mid)

        u_out = step - lag - hops

        @pl.when((u_out >= 0) & (u_out < units))
        def _():
            home(u_out)

        u_last = step - lag - hops - 2

        @pl.when(u_last >= 0)
        def _():
            blend(u_last)

        return carry

    lax.fori_loop(0, units + lag + hops + 2, slot, 0)
    out = hidden[...]
    layer_out[...] = out.astype(bf16)
    message = jnp.where(lane == 0, lane_sum(out * out), 0.0)
    message = jnp.where(lane == 1, lane_sum(out * (final_gain[...] * value_weight[...])), message)
    total = both(1, message)
    estimate = total[:, 1:2] * lax.rsqrt(total[:, 0:1] / full_width + eps) + value_bias[0]
    real = (z * nx + x) * count + row < limit
    flat = jnp.sum(jnp.where((lane == row) & real, estimate, 0.0), axis=0, keepdims=True)
    values[...] = flat

    def drain(u, carry):
        rows_drain(u)
        ups_copy(u).wait_send()
        twin_copy(u).wait_send()
        act_copy(u).wait_send()
        for b in (0, 1):

            @pl.when((u > 0) | (c != b))
            def _():
                back_copy(b, u).wait_send()

        for way in (0, 1):
            for k in range(1, hops):
                g_copy(way, u, k).wait_send()
                r_copy(way, u, k, own(way, u, k)).wait_send()

            @pl.when(lax.rem(u, 2) == way)
            def _():
                g_copy(way, u, hops).wait_send()
                r_copy(way, u, 0, own(way, u, 0)).wait_send()

        return carry

    lax.fori_loop(0, units, drain, 0)
    for k in range(2 * chunks):
        weight_copy(k).wait_send()


def on_device(dims, *args):
    (stream, queries, key_rows, value_rows, routes, seq_length, norm_gain, router) = args[:8]
    (w_up, w_down, final_gain, value_weight, value_bias) = args[8:]
    nz, nx, _ = dims
    units, hops = nz // 2, nx // 2
    count, width = stream.shape
    hid, narrow = w_up.shape[1], width // 2
    heads = key_rows.shape[1] // HD
    mine = nx * count
    stacked = width // nx // HD * mine
    vmem, smem, far = (
        pl.BlockSpec(memory_space=pltpu.VMEM),
        pl.BlockSpec(memory_space=pltpu.SMEM),
        pl.BlockSpec(memory_space=pl.ANY),
    )
    dma = pltpu.SemaphoreType.DMA
    layer_out, values = pl.pallas_call(
        functools.partial(kernel, dims),
        out_shape=(
            jax.ShapeDtypeStruct((count, width), bf16),
            jax.ShapeDtypeStruct((1, META), f32),
        ),
        in_specs=[vmem, vmem, vmem, vmem, vmem, smem, vmem, vmem, far, far, vmem, vmem, smem],
        out_specs=(vmem, vmem),
        scratch_shapes=[
            pltpu.VMEM((nx, count, width // nx), bf16),
            pltpu.VMEM((heads, count, 2 * HD), bf16),
            pltpu.VMEM((units, 2, nx, count, 2 * HD), bf16),
            pltpu.VMEM((nx, count, width // nx), bf16),
            pltpu.VMEM((nx, count, width // nx), bf16),
            pltpu.VMEM((stacked, HD), f32),
            pltpu.VMEM((stacked, HD), f32),
            pltpu.VMEM((stacked, HD), f32),
            pltpu.VMEM((count, narrow + META), bf16),
            pltpu.VMEM((units, 2, count, narrow + META), bf16),
            pltpu.VMEM((units, nx, count, narrow), bf16),
            pltpu.VMEM((count, width), f32),
            pltpu.VMEM((2, count, META), f32),
            pltpu.VMEM((narrow, hid), bf16),
            pltpu.VMEM((hid, narrow), bf16),
            pltpu.VMEM((narrow, hid), bf16),
            pltpu.VMEM((hid, narrow), bf16),
            pltpu.VMEM((2, count, META), f32),
            pltpu.VMEM((2, count, META), f32),
            pltpu.VMEM((units, mine, hid), f32),
            pltpu.VMEM((units, mine, hid), bf16),
            pltpu.VMEM((units, mine, hid), bf16),
            pltpu.VMEM((units, mine, hid), f32),
            pltpu.VMEM((units, mine, hid), f32),
            pltpu.VMEM((units, mine, hid), bf16),
            pltpu.VMEM((units, mine, hid), bf16),
            pltpu.VMEM((units, nx, count, narrow), bf16),
            pltpu.VMEM((2, units, hops, count, narrow), bf16),
            pltpu.VMEM((2, units, hops, count, narrow), bf16),
            pltpu.VMEM((units, 2, count // 2, narrow), bf16),
            pltpu.VMEM((units, 2, count // 2, narrow), bf16),
            dma((2,)),
            dma((3, nx)),
            dma((3, nx)),
            dma((2, units)),
            dma((2, 2, units)),
            dma((2, 2, units, hops)),
            dma((2, 2, units, hops)),
            dma((2, units)),
            dma((2, units)),
            dma((2,)),
            dma((2,)),
            dma((3, units)),
            dma((3, units)),
            dma((2 * chunks,)),
            dma((2 * chunks,)),
        ],
        compiler_params=pltpu.CompilerParams(
            collective_id=0, has_side_effects=True, vmem_limit_bytes=56 * 2**20
        ),
        name="layer",
    )(
        queries,
        key_rows,
        value_rows,
        stream,
        routes.T,
        seq_length,
        norm_gain.reshape(1, width),
        router.T,
        w_up,
        w_down,
        final_gain.reshape(1, width),
        value_weight.reshape(1, width),
        value_bias,
    )
    return layer_out, values[0, :count]


def build(mesh, nz, nx, full_width):
    finer = Mesh(
        mesh.devices.reshape(mesh.shape["groups"], nz, nx, mesh.shape["tp"]),
        ("groups", "z", "x", "tp"),
    )
    placed = (
        P(GROUPS_SEQ, "tp"),
        P(GROUPS_SEQ, "tp"),
        P(GROUPS_SEQ, "tp"),
        P(GROUPS_SEQ, "tp"),
        P(GROUPS_SEQ, None),
        P("groups"),
        P("tp"),
        P("tp", None),
        P("tp", SEQ),
        P(SEQ, "tp"),
        P("tp"),
        P("tp"),
        P(),
    )
    return jax.shard_map(
        functools.partial(on_device, (nz, nx, full_width)),
        mesh=finer,
        in_specs=placed,
        out_specs=(P(GROUPS_SEQ, "tp"), P(GROUPS_SEQ)),
        check_vma=False,
    )


def solution(mesh):
    return build(mesh, 16, mesh.shape["seq"] // 16, 6144)
```

```python
import functools
import math

import jax
import jax.numpy as jnp
from jax import lax
from jax.experimental import pallas as pl
from jax.experimental.pallas import tpu as pltpu
from jax.sharding import Mesh
from jax.sharding import PartitionSpec as P

HD = 128
EXPERTS = 4
META = 128
SEQ = ("z", "x")
GROUPS_SEQ = ("groups", "z", "x")
eps = 1e-05
masked = -1e30
chunks = 8
f32 = jnp.float32
bf16 = jnp.bfloat16


def lane_sum(a):
    return jnp.sum(a, axis=1, keepdims=True)


def kernel(
    dims,
    queries,
    key_rows,
    value_rows,
    stream,
    routes,
    seq_length,
    norm_gain,
    router,
    w_up_hbm,
    w_down_hbm,
    final_gain,
    value_weight,
    value_bias,
    layer_out,
    values,
    q_all,
    kv_own,
    kv,
    att_out,
    att_in,
    top_score,
    weight_sum,
    mixed_values,
    rows_out,
    rows_z,
    rows_x,
    hidden,
    info,
    w_up,
    w_down,
    w_up_in,
    stats,
    stats_in,
    ups,
    ups_out,
    ups_in,
    ups_twin,
    parts,
    sums,
    recv,
    back_out,
    back_in,
    local_sem,
    asend,
    arecv,
    zsend,
    zrecv,
    xsend,
    xrecv,
    bsend,
    brecv,
    tsend,
    trecv,
    usend,
    urecv,
    wsend,
    wrecv,
):
    nz, nx, full_width = dims
    units, hops = nz // 2, nx // 2
    z, x, t = lax.axis_index("z"), lax.axis_index("x"), lax.axis_index("tp")
    right, left = {"x": lax.rem(x + 1, nx)}, {"x": lax.rem(x + nx - 1, nx)}
    twin = {"tp": 1 - t}
    count, width = stream.shape
    kv_width = key_rows.shape[1]
    q_width = width // nx
    sharers = nx // (kv_width // HD)

    def along_z(steps):
        return {"z": lax.rem(z + nz + steps, nz)}

    def remote(src, dst, send, recv, to):
        return pltpu.make_async_remote_copy(
            src_ref=src, dst_ref=dst, send_sem=send, recv_sem=recv, device_id=to,
            device_id_type=pl.DeviceIdType.MESH,
        )

    c = lax.rem(z, 2)
    m, pairs = z // 2, nz // 2
    narrow, hid = width // 2, w_up_hbm.shape[1]
    mate = {"z": z + 1 - 2 * c}
    keep_rows = pl.ds(pl.multiple_of(c * narrow, HD), narrow)
    up_copy = pltpu.make_async_copy(w_up_hbm.at[keep_rows, :], w_up, local_sem.at[0])
    down_copy = pltpu.make_async_copy(w_down_hbm, w_down, local_sem.at[1])

    def weight_copy(k):
        size = narrow // chunks
        at = pl.ds(pl.multiple_of((1 - c) * narrow + k * size, HD // 4), size)
        return remote(w_up_hbm.at[at, :], w_up_in.at[pl.ds(k * size, size), :], wsend.at[k], wrecv.at[k], mate)

    up_copy.start()
    down_copy.start()
    barrier = pltpu.get_barrier_semaphore()

    def greet(peer):
        pl.semaphore_signal(barrier, inc=1, device_id=peer, device_id_type=pl.DeviceIdType.MESH)

    kv[...] = jnp.zeros(kv.shape, bf16)
    for steps in (1, -1, 2, -2):
        greet(along_z(steps))
    for d in range(1, nx):
        greet({"x": lax.rem(x + d, nx)})
    diagonal = {**mate, **twin}
    greet(twin)
    greet(diagonal)
    for head in range(kv_width // HD):
        kv_own[head, :, :HD] = key_rows[:, head * HD : (head + 1) * HD]
        kv_own[head, :, HD:] = value_rows[:, head * HD : (head + 1) * HD]
    kv[0, 0, x] = kv_own[x // sharers]
    q_all[x] = queries[:, pl.ds(pl.multiple_of(x * q_width, HD), q_width)]
    pl.semaphore_wait(barrier, 5 + nx)

    def q_copy(d):
        peer = lax.rem(x + d, nx)
        at = pl.ds(pl.multiple_of(peer * q_width, HD), q_width)
        return remote(queries.at[:, at], q_all.at[x], asend.at[0, d], arecv.at[0, d], {"x": peer})

    def kv_copy(d):
        peer = lax.rem(x + d, nx)
        return remote(kv_own.at[peer // sharers], kv.at[0, 0, x], asend.at[1, d], arecv.at[1, d], {"x": peer})

    def att_copy(d):
        peer = lax.rem(x + d, nx)
        return remote(att_out.at[peer], att_in.at[x], asend.at[2, d], arecv.at[2, d], {"x": peer})

    far_first = sorted(range(1, nx), key=lambda d: -min(d, nx - d))
    for d in far_first:
        kv_copy(d).start()
    for d in far_first:
        q_copy(d).start()

    def wanted(way, u, steps):
        at = lax.rem(z + nz + steps, nz)
        if way == 1:
            return at > u
        return (at + u >= nz) | (u + 2 * (at // 2) + 2 < units)

    def kv_copy_z(way, u, src, steps):
        return remote(src, kv.at[u, way], zsend.at[0, way, u], zrecv.at[0, way, u], along_z(steps))

    def kv_first(way, u):
        steps = -u if way == 0 else u + 1
        return kv_copy_z(way, u, kv.at[0, 0], steps), wanted(way, u, steps)

    def kv_onward(way, u):
        steps = -2 if way == 0 else 2
        return kv_copy_z(way, u, kv.at[lax.max(u - 2, 0), way], steps), wanted(way, u, steps)

    def kv_start():
        for way, u in ((1, 1), (0, 2), (1, 0), (0, 1)):
            copy, needed = kv_first(way, u)
            pl.when(needed)(copy.start)

    def kv_take(u):
        for way in (1, 0):

            @pl.when(wanted(way, u, 0) & ((u > 0) | (way == 1)))
            def _():
                kv_onward(way, u)[0].wait_recv()

            copy, needed = kv_onward(way, u + 2)
            pl.when(needed & (u + 2 < units) & ((u > 0) | (way == 1)))(copy.start)

    def kv_drain(u):
        for way in (0, 1):
            steps = (-1 if way == 0 else 1) * jnp.minimum(u + way, 2)
            pl.when(wanted(way, u, steps) & ((u > 0) | (way == 1)))(kv_onward(way, u)[0].wait_send)

    for d in range(1, nx):
        kv_copy(d).wait_recv()
    kv_start()
    for d in range(1, nx):
        q_copy(d).wait_recv()

    mine = nx * count
    per = q_width // HD
    limit = seq_length[0]
    top_score[...] = jnp.full(top_score.shape, masked, f32)
    weight_sum[...] = jnp.zeros(weight_sum.shape, f32)
    mixed_values[...] = jnp.zeros(mixed_values.shape, f32)
    q_row = lax.broadcasted_iota(jnp.int32, (per * mine, 2 * mine), 0)
    k_row = lax.broadcasted_iota(jnp.int32, (per * mine, 2 * mine), 1)
    q_pos = z * mine + lax.rem(q_row, mine)

    def attend(u, carry):
        kv_take(u)
        q = jnp.concatenate(
            [q_all[:, :, j * HD : (j + 1) * HD].reshape(mine, HD) for j in range(per)], axis=0
        )
        k = kv[u, :, :, :, :HD].reshape(2 * mine, HD)
        v = kv[u, :, :, :, HD:].reshape(2 * mine, HD)
        s = lax.dot_general(q, k, (((1,), (1,)), ((), ())), preferred_element_type=f32) * (1.0 / math.sqrt(HD))
        k_pos = jnp.where(
            k_row < mine, lax.rem(z + u, nz) * mine + k_row, lax.rem(z - u - 1 + nz, nz) * mine + k_row - mine
        )
        allowed = (k_pos <= q_pos) & (k_pos < limit)
        s = jnp.where(allowed, s, masked)
        old = top_score[:, 0:1]
        new = jnp.maximum(old, jnp.max(s, axis=1, keepdims=True))
        p = jnp.where(allowed, jnp.exp(s - new), 0.0)
        keep = jnp.exp(old - new)
        top_score[...] = jnp.broadcast_to(new, top_score.shape)
        weight_sum[...] = weight_sum[...] * keep + lane_sum(p)
        mixed_values[...] = mixed_values[...] * keep + jnp.dot(p.astype(bf16), v, preferred_element_type=f32)
        return carry

    for u in range(units):
        attend(u, 0)
    ahead = chunks - 3
    for k in range(ahead):
        weight_copy(k).start()
    attended = mixed_values[...] / weight_sum[...]
    for s in range(nx):
        for j in range(per):
            piece = attended[j * mine + s * count : j * mine + (s + 1) * count]
            att_out[s, :, j * HD : (j + 1) * HD] = piece.astype(bf16)
    att_in[x] = att_out[x]
    for d in far_first:
        att_copy(d).start()
    for d in range(1, nx):
        kv_copy(d).wait_send()
        q_copy(d).wait_send()
    for d in range(1, nx):
        att_copy(d).wait_recv()
    for s in range(nx):
        at = slice(s * q_width, (s + 1) * q_width)
        hidden[:, at] = stream[:, at].astype(f32) + att_in[s].astype(f32)

    def both(index, message):
        stats[index] = message
        copy = remote(stats.at[index], stats_in.at[index], tsend.at[index], trecv.at[index], twin)
        copy.start()
        copy.wait()
        return message + stats_in[index]

    lane = lax.broadcasted_iota(jnp.int32, (count, META), 1)
    row = lax.broadcasted_iota(jnp.int32, (count, META), 0)

    def upright(line):
        return lane_sum(jnp.where(lane == row, jnp.broadcast_to(line, (count, META)), 0.0))

    h_all = hidden[...]
    gained = h_all * norm_gain[...]
    message = jnp.where(lane == EXPERTS, lane_sum(h_all * h_all), 0.0)
    for e in range(EXPERTS):
        message = jnp.where(lane == e, lane_sum(gained * router[e : e + 1]), message)
    total = both(0, message)
    sq = lane_sum(jnp.where(lane == EXPERTS, total, 0.0))
    scale = lax.rsqrt(sq / full_width + eps)
    logits = total * scale
    spread = jnp.concatenate([routes[...].astype(f32), jnp.zeros((2, META - count), f32)], axis=1)
    first, second = upright(spread[0:1]).astype(jnp.int32), upright(spread[1:2]).astype(jnp.int32)
    hit_a, hit_b = lane == first, lane == second
    gap = lane_sum(jnp.where(hit_a, logits, 0.0)) - lane_sum(jnp.where(hit_b, logits, 0.0))
    gate_a, gate_b = 1.0 / (1.0 + jnp.exp(-gap)), 1.0 / (1.0 + jnp.exp(gap))
    hits = jnp.where(hit_a | hit_b, 1.0, 0.0)
    rank = jnp.zeros((count, META), f32)
    for i in range(count - 1):
        rank = rank + jnp.where(row > i, jnp.broadcast_to(hits[i : i + 1], (count, META)), 0.0)
    place = jnp.where(hits > 0.5, rank + 1.0, 0.0)
    normed = gained * scale
    low, high = normed[:, :narrow], normed[:, narrow:]
    rows_out[:, :narrow] = jnp.where(c == 0, high, low).astype(bf16)
    rows_out[:, narrow:] = place.astype(bf16)
    rows_z[0, c, :, :narrow] = jnp.where(c == 0, low, high).astype(bf16)
    rows_z[0, c, :, narrow:] = place.astype(bf16)

    def mate_rows():
        return remote(rows_out, rows_z.at[0, c], zsend.at[1, 0, 0], zrecv.at[1, 0, 0], mate)

    def rows_copy(b, u):
        return remote(
            rows_z.at[lax.max(u - 2, 0), b], rows_z.at[u, b], zsend.at[1, b, u], zrecv.at[1, b, u],
            along_z(2 - 4 * lax.rem(u, 2)),
        )

    mate_rows().start()

    def rows_take(u):
        @pl.when(u == 0)
        def _():
            mate_rows().wait_recv()
            for b in (0, 1):
                rows_copy(b, 1).start()
                rows_copy(b, 2).start()

        @pl.when(u > 0)
        def _():
            for b in (0, 1):
                rows_copy(b, u).wait_recv()

                @pl.when(u + 2 < units)
                def _():
                    rows_copy(b, u + 2).start()

    def rows_drain(u):
        @pl.when(u == 0)
        def _():
            mate_rows().wait_send()

        @pl.when(u > 0)
        def _():
            for b in (0, 1):
                rows_copy(b, u).wait_send()

    info[0] = place
    info[1] = jnp.where(hit_a, gate_a, jnp.where(hit_b, gate_b, 0.0))

    ringed, chained = units, units
    my_expert = z // (nz // EXPERTS)
    slots = count // 2

    def column(table, expert):
        return lane_sum(jnp.where(lane == expert, table, 0.0))

    def choose(u):
        out = jnp.zeros((count, narrow), f32)
        for half in (0, 1):
            block = rows_z[u, half].astype(f32)
            places = jnp.broadcast_to(column(block[:, narrow:], my_expert), (count, META))
            for i in range(count):
                want = jnp.broadcast_to(places[i : i + 1], (count, META)) + (slots * half)
                chosen = jnp.where(((row + 1).astype(f32) == want) & (want > slots * half + 0.5), 1.0, 0.0)
                out = out + chosen[:, 0:1] * block[i : i + 1, :narrow]
        rows_x[u, x] = out.astype(bf16)

    def g_copy(way, u, h):
        back = nx - (h - 1) if way == 0 else h - 1
        at = rows_x.at[u, lax.rem(x + back, nx)]
        return remote(
            at, at, xsend.at[0, way, u, h - 1], xrecv.at[0, way, u, h - 1], right if way == 0 else left
        )

    def ups_copy(u):
        return remote(ups_out.at[u], ups_in.at[0, u], usend.at[0, u], urecv.at[0, u], mate)

    def cross_copy(u):
        return remote(ups_out.at[u], ups_in.at[1, u], usend.at[3, u], urecv.at[3, u], diagonal)

    def twin_copy(u):
        return remote(ups.at[u], ups_twin.at[u], usend.at[1, u], urecv.at[1, u], twin)

    def project(u):
        got = rows_x[u].reshape(mine, narrow)
        ups_out[u] = jnp.dot(got, w_up_in[...], preferred_element_type=f32).astype(bf16)
        ups_copy(u).start()
        cross_copy(u).start()
        ups[u] = jnp.dot(got, w_up[...], preferred_element_type=f32)
        twin_copy(u).start()

    def way_of(d):
        return (0, d) if d <= hops else (1, nx - d)

    def wide_copy(u, d):
        way, h = way_of(d)
        at = rows_x.at[u, x]
        return remote(
            at, at, xsend.at[0, way, u, h - 1], xrecv.at[0, way, u, h - 1], {"x": lax.rem(x + d, nx)}
        )

    def part_copy(u, d):
        way, h = way_of(d)
        peer = lax.rem(x + d, nx)
        return remote(
            parts.at[u, peer], recv.at[way, u, h - 1], xsend.at[1, way, u, h - 1], xrecv.at[1, way, u, h - 1],
            {"x": peer},
        )

    def own(way, u, k):
        ahead = hops - k
        return parts.at[u, lax.rem(x + (ahead if way == 0 else nx - ahead), nx)]

    def r_copy(way, u, k, src):
        return remote(
            src, recv.at[way, u, k], xsend.at[1, way, u, k], xrecv.at[1, way, u, k], right if way == 0 else left
        )

    def expand(u):
        ups_copy(u).wait_recv()
        cross_copy(u).wait_recv()
        twin_copy(u).wait_recv()
        v = ups[u] + ups_twin[u] + (ups_in[0, u].astype(f32) + ups_in[1, u].astype(f32))
        active = (v / (1.0 + jnp.exp(-v))).astype(bf16)
        made = jnp.dot(active, w_down[...], preferred_element_type=f32)
        for d in range(nx):
            parts[u, d] = made[d * count : (d + 1) * count].astype(bf16)

        @pl.when(u < chained)
        def _():
            for way in (0, 1):

                @pl.when(lax.rem(u, 2) == way)
                def _():
                    r_copy(way, u, 0, own(way, u, 0)).start()

        @pl.when(u >= chained)
        def _():
            for d in far_first:
                part_copy(u, d).start()

    def offset(u):
        return ((u + 1) // 2) * (2 * lax.rem(u, 2) - 1)

    def back_copy(b, u):
        to = {"z": 2 * lax.rem(m + offset(u) + pairs, pairs) + b}
        return remote(back_out.at[u, b], back_in.at[u, c], bsend.at[b, u], brecv.at[c, u], to)

    def back_arrival(b, u):
        to = {"z": 2 * lax.rem(m + offset(u) + pairs, pairs) + b}
        return remote(back_out.at[u, b], back_in.at[u, b], bsend.at[b, u], brecv.at[b, u], to)

    def home(u):
        def settle(total):
            done = total.astype(bf16)
            back_in_or_out(u, done)

        @pl.when(u < chained)
        def _():
            for way in (0, 1):
                r_copy(way, u, hops - 1, own(way, u, hops - 1)).wait_recv()
            both_ways = recv[0, u, hops - 1].astype(f32) + recv[1, u, hops - 1].astype(f32)
            settle(parts[u, x].astype(f32) + both_ways)

        @pl.when(u >= chained)
        def _():
            total = parts[u, x].astype(f32)
            for d in range(1, nx):
                part_copy(u, d).wait_recv()
                way, h = way_of(d)
                total = total + recv[way, u, h - 1].astype(f32)
            settle(total)

    def back_in_or_out(u, done):
        for b in (0, 1):
            back_out[u, b] = done[b * slots : (b + 1) * slots]

            @pl.when((u > 0) | (c != b))
            def _():
                back_copy(b, u).start()

            @pl.when((u == 0) & (c == b))
            def _():
                back_in[0, b] = done[b * slots : (b + 1) * slots]

    def blend(u):
        source = lax.rem(m - offset(u) + pairs, pairs)
        expert = 2 * source // (nz // EXPERTS)
        places, gate = column(info[0], expert), column(info[1], expert)
        weights = [jnp.where(places == float(i + 1), gate, 0.0) for i in range(slots)]
        for b in (0, 1):

            @pl.when((u > 0) | (c != b))
            def _():
                back_arrival(b, u).wait_recv()

            got = back_in[u, b].astype(f32)
            mix = hidden[...]
            for i in range(slots):
                mix = mix + weights[i] * got[i : i + 1]
            hidden[...] = mix

    for d in range(1, nx):
        att_copy(d).wait_send()
    up_copy.wait()
    down_copy.wait()
    groups = ((0, units, hops, hops),)

    def staged(step, delay, work):
        for low, high, start, end in groups:
            u = step - start - (delay if delay < 2 else delay - 1 + end)
            pl.when((u >= low) & (u < high))(functools.partial(work, u))

    def collect(u):
        @pl.when(u < ringed)
        def _():
            for way in (0, 1):

                @pl.when(lax.rem(u, 2) == way)
                def _():
                    g_copy(way, u, hops).wait_recv()

        @pl.when(u >= ringed)
        def _():
            for d in range(1, nx):
                way, h = way_of(d)
                g_copy(way, u, h).wait_recv()

        project(u)

    first_project = min(hops, ringed + 1)

    def slot(step, carry):
        @pl.when(step < units)
        def _():
            rows_take(step)
            choose(step)

            @pl.when(step == units - 1)
            def _():
                for d in range(1, nz):
                    greet(along_z(d))

            @pl.when(step < ringed)
            def _():
                g_copy(0, step, 1).start()
                g_copy(1, step, 1).start()

            @pl.when(step >= ringed)
            def _():
                for d in far_first:
                    wide_copy(step, d).start()

        for k in range(ahead, chunks):

            @pl.when(step == max(0, first_project - 4) + k - ahead)
            def _():
                weight_copy(k).start()

        for h in range(1, hops):
            u = step - h

            @pl.when((u >= 0) & (u < ringed))
            def _():
                for way in (0, 1):
                    g_copy(way, u, h).wait_recv()
                    if h < hops - 1:
                        g_copy(way, u, h + 1).start()
                    else:

                        @pl.when(lax.rem(u, 2) == way)
                        def _():
                            g_copy(way, u, h + 1).start()

        for k in range(1, hops):
            u = step - hops - 1 - k

            @pl.when((u >= 0) & (u < chained))
            def _():
                for way in (0, 1):

                    def add():
                        r_copy(way, u, k - 1, own(way, u, k - 1)).wait_recv()
                        total = recv[way, u, k - 1].astype(f32) + own(way, u, k)[...].astype(f32)
                        sums[way, u, k] = total.astype(bf16)
                        r_copy(way, u, k, sums.at[way, u, k]).start()

                    if k > 1:
                        add()
                    else:
                        pl.when(lax.rem(u, 2) == way)(add)

                        @pl.when(lax.rem(u, 2) != way)
                        def _():
                            r_copy(way, u, k, own(way, u, k)).start()

        first_home = min(low + start + 1 + end for low, high, start, end in groups)

        @pl.when(step == first_home)
        def _():
            pl.semaphore_wait(barrier, nz - 1)

        @pl.when(step == first_project)
        def _():
            for k in range(chunks):
                weight_copy(k).wait_recv()

        staged(step, 0, collect)
        staged(step, 1, expand)
        staged(step, 2, home)
        staged(step, 4, blend)
        return carry

    last = max(high - 1 + start + 3 + end for low, high, start, end in groups)
    lax.fori_loop(0, last + 1, slot, 0)
    out = hidden[...]
    layer_out[...] = out.astype(bf16)
    message = jnp.where(lane == 0, lane_sum(out * out), 0.0)
    message = jnp.where(lane == 1, lane_sum(out * (final_gain[...] * value_weight[...])), message)
    total = both(1, message)
    estimate = total[:, 1:2] * lax.rsqrt(total[:, 0:1] / full_width + eps) + value_bias[0]
    real = (z * nx + x) * count + row < limit
    flat = jnp.sum(jnp.where((lane == row) & real, estimate, 0.0), axis=0, keepdims=True)
    values[...] = flat

    def drain(u, carry):
        kv_drain(u)
        rows_drain(u)
        ups_copy(u).wait_send()
        twin_copy(u).wait_send()
        cross_copy(u).wait_send()
        for b in (0, 1):

            @pl.when((u > 0) | (c != b))
            def _():
                back_copy(b, u).wait_send()

        for way in (0, 1):
            even = lax.rem(u, 2) == way
            for k in range(1, hops):
                g_copy(way, u, k).wait_send()
            for k in range(1, hops if way == 0 else hops - 1):
                r_copy(way, u, k, own(way, u, k)).wait_send()
            one_way = (u < ringed) & even
            pl.when(one_way | (u >= ringed) if way == 0 else one_way)(g_copy(way, u, hops).wait_send)
            pl.when(((u < chained) & even) | (u >= chained))(r_copy(way, u, 0, own(way, u, 0)).wait_send)
            if way == 1:
                pl.when(u < chained)(r_copy(way, u, hops - 1, own(way, u, hops - 1)).wait_send)

        return carry

    lax.fori_loop(0, units, drain, 0)
    for k in range(chunks):
        weight_copy(k).wait_send()


def on_device(dims, *args):
    (stream, queries, key_rows, value_rows, routes, seq_length, norm_gain, router) = args[:8]
    (w_up, w_down, final_gain, value_weight, value_bias) = args[8:]
    nz, nx, _ = dims
    units, hops = nz // 2, nx // 2
    count, width = stream.shape
    hid, narrow = w_up.shape[1], width // 2
    heads = key_rows.shape[1] // HD
    mine = nx * count
    stacked = width // nx // HD * mine
    vmem, smem, far = (
        pl.BlockSpec(memory_space=pltpu.VMEM),
        pl.BlockSpec(memory_space=pltpu.SMEM),
        pl.BlockSpec(memory_space=pl.ANY),
    )
    dma = pltpu.SemaphoreType.DMA
    layer_out, values = pl.pallas_call(
        functools.partial(kernel, dims),
        out_shape=(
            jax.ShapeDtypeStruct((count, width), bf16),
            jax.ShapeDtypeStruct((1, META), f32),
        ),
        in_specs=[vmem, vmem, vmem, vmem, vmem, smem, vmem, vmem, far, far, vmem, vmem, smem],
        out_specs=(vmem, vmem),
        scratch_shapes=[
            pltpu.VMEM((nx, count, width // nx), bf16),
            pltpu.VMEM((heads, count, 2 * HD), bf16),
            pltpu.VMEM((units, 2, nx, count, 2 * HD), bf16),
            pltpu.VMEM((nx, count, width // nx), bf16),
            pltpu.VMEM((nx, count, width // nx), bf16),
            pltpu.VMEM((stacked, HD), f32),
            pltpu.VMEM((stacked, HD), f32),
            pltpu.VMEM((stacked, HD), f32),
            pltpu.VMEM((count, narrow + META), bf16),
            pltpu.VMEM((units, 2, count, narrow + META), bf16),
            pltpu.VMEM((units, nx, count, narrow), bf16),
            pltpu.VMEM((count, width), f32),
            pltpu.VMEM((2, count, META), f32),
            pltpu.VMEM((narrow, hid), bf16),
            pltpu.VMEM((hid, width), bf16),
            pltpu.VMEM((narrow, hid), bf16),
            pltpu.VMEM((2, count, META), f32),
            pltpu.VMEM((2, count, META), f32),
            pltpu.VMEM((units, mine, hid), f32),
            pltpu.VMEM((units, mine, hid), bf16),
            pltpu.VMEM((2, units, mine, hid), bf16),
            pltpu.VMEM((units, mine, hid), f32),
            pltpu.VMEM((units, nx, count, width), bf16),
            pltpu.VMEM((2, units, hops, count, width), bf16),
            pltpu.VMEM((2, units, hops, count, width), bf16),
            pltpu.VMEM((units, 2, count // 2, width), bf16),
            pltpu.VMEM((units, 2, count // 2, width), bf16),
            dma((2,)),
            dma((3, nx)),
            dma((3, nx)),
            dma((2, 2, units)),
            dma((2, 2, units)),
            dma((2, 2, units, hops)),
            dma((2, 2, units, hops)),
            dma((2, units)),
            dma((2, units)),
            dma((2,)),
            dma((2,)),
            dma((4, units)),
            dma((4, units)),
            dma((chunks,)),
            dma((chunks,)),
        ],
        compiler_params=pltpu.CompilerParams(
            collective_id=0, has_side_effects=True, vmem_limit_bytes=56 * 2**20
        ),
        name="layer",
    )(
        queries,
        key_rows,
        value_rows,
        stream,
        routes.T,
        seq_length,
        norm_gain.reshape(1, width),
        router.T,
        w_up,
        w_down,
        final_gain.reshape(1, width),
        value_weight.reshape(1, width),
        value_bias,
    )
    return layer_out, values[0, :count]


def build(mesh, nz, nx, full_width):
    finer = Mesh(
        mesh.devices.reshape(mesh.shape["groups"], nz, nx, mesh.shape["tp"]),
        ("groups", "z", "x", "tp"),
    )
    placed = (
        P(GROUPS_SEQ, "tp"),
        P(GROUPS_SEQ, "tp"),
        P(GROUPS_SEQ, "tp"),
        P(GROUPS_SEQ, "tp"),
        P(GROUPS_SEQ, None),
        P("groups"),
        P("tp"),
        P("tp", None),
        P("tp", SEQ),
        P(SEQ, "tp"),
        P("tp"),
        P("tp"),
        P(),
    )
    return jax.shard_map(
        functools.partial(on_device, (nz, nx, full_width)),
        mesh=finer,
        in_specs=placed,
        out_specs=(P(GROUPS_SEQ, "tp"), P(GROUPS_SEQ)),
        check_vma=False,
    )


def solution(mesh):
    return build(mesh, 16, mesh.shape["seq"] // 16, 6144)
```

```python
import functools
import math

import jax
import jax.numpy as jnp
from jax import lax
from jax.experimental import pallas as pl
from jax.experimental.pallas import tpu as pltpu
from jax.sharding import Mesh
from jax.sharding import PartitionSpec as P

HD = 128
EXPERTS = 4
META = 128
SEQ = ("z", "x")
GROUPS_SEQ = ("groups", "z", "x")
eps = 1e-05
masked = -1e30
chunks = 8
f32 = jnp.float32
bf16 = jnp.bfloat16


def lane_sum(a):
    return jnp.sum(a, axis=1, keepdims=True)


def kernel(
    dims,
    queries,
    key_rows,
    value_rows,
    stream,
    routes,
    seq_length,
    norm_gain,
    router,
    w_up_hbm,
    w_down_hbm,
    final_gain,
    value_weight,
    value_bias,
    layer_out,
    values,
    q_all,
    kv_own,
    kv,
    att_out,
    att_in,
    top_score,
    weight_sum,
    mixed_values,
    rows_out,
    rows_z,
    rows_x,
    hidden,
    info,
    w_up,
    w_down,
    w_up_in,
    stats,
    stats_in,
    ups,
    ups_out,
    ups_in,
    ups_twin,
    parts,
    sums,
    recv,
    back_out,
    back_in,
    local_sem,
    asend,
    arecv,
    zsend,
    zrecv,
    xsend,
    xrecv,
    bsend,
    brecv,
    tsend,
    trecv,
    usend,
    urecv,
    wsend,
    wrecv,
):
    nz, nx, full_width = dims
    units, hops = nz // 2, nx // 2
    z, x, t = lax.axis_index("z"), lax.axis_index("x"), lax.axis_index("tp")
    right, left = {"x": lax.rem(x + 1, nx)}, {"x": lax.rem(x + nx - 1, nx)}
    twin = {"tp": 1 - t}
    count, width = stream.shape
    kv_width = key_rows.shape[1]
    q_width = width // nx
    sharers = nx // (kv_width // HD)

    def along_z(steps):
        return {"z": lax.rem(z + nz + steps, nz)}

    def remote(src, dst, send, recv, to):
        return pltpu.make_async_remote_copy(
            src_ref=src, dst_ref=dst, send_sem=send, recv_sem=recv, device_id=to,
            device_id_type=pl.DeviceIdType.MESH,
        )

    c = lax.rem(z, 2)
    m, pairs = z // 2, nz // 2
    narrow, hid = width // 2, w_up_hbm.shape[1]
    mate = {"z": z + 1 - 2 * c}
    keep_rows = pl.ds(pl.multiple_of(c * narrow, HD), narrow)
    up_copy = pltpu.make_async_copy(w_up_hbm.at[keep_rows, :], w_up, local_sem.at[0])
    down_copy = pltpu.make_async_copy(w_down_hbm, w_down, local_sem.at[1])

    def weight_copy(k):
        size = narrow // chunks
        at = pl.ds(pl.multiple_of((1 - c) * narrow + k * size, HD // 4), size)
        return remote(w_up_hbm.at[at, :], w_up_in.at[pl.ds(k * size, size), :], wsend.at[k], wrecv.at[k], mate)

    up_copy.start()
    down_copy.start()
    barrier = pltpu.get_barrier_semaphore()

    def greet(peer):
        pl.semaphore_signal(barrier, inc=1, device_id=peer, device_id_type=pl.DeviceIdType.MESH)

    kv[...] = jnp.zeros(kv.shape, bf16)
    for steps in (1, -1, 2, -2):
        greet(along_z(steps))
    for d in range(1, nx):
        greet({"x": lax.rem(x + d, nx)})
    diagonal = {**mate, **twin}
    greet(twin)
    greet(diagonal)
    for head in range(kv_width // HD):
        kv_own[head, :, :HD] = key_rows[:, head * HD : (head + 1) * HD]
        kv_own[head, :, HD:] = value_rows[:, head * HD : (head + 1) * HD]
    kv[0, 0, x] = kv_own[x // sharers]
    q_all[x] = queries[:, pl.ds(pl.multiple_of(x * q_width, HD), q_width)]
    pl.semaphore_wait(barrier, 5 + nx)

    def q_copy(d):
        peer = lax.rem(x + d, nx)
        at = pl.ds(pl.multiple_of(peer * q_width, HD), q_width)
        return remote(queries.at[:, at], q_all.at[x], asend.at[0, d], arecv.at[0, d], {"x": peer})

    def kv_copy(d):
        peer = lax.rem(x + d, nx)
        return remote(kv_own.at[peer // sharers], kv.at[0, 0, x], asend.at[1, d], arecv.at[1, d], {"x": peer})

    def att_copy(d):
        peer = lax.rem(x + d, nx)
        return remote(att_out.at[peer], att_in.at[x], asend.at[2, d], arecv.at[2, d], {"x": peer})

    far_first = sorted(range(1, nx), key=lambda d: -min(d, nx - d))
    for d in far_first:
        kv_copy(d).start()
    for d in far_first:
        q_copy(d).start()

    def wanted(way, u, steps):
        at = lax.rem(z + nz + steps, nz)
        if way == 1:
            return at > u
        return (at + u >= nz) | (u + 2 * (at // 2) + 2 < units)

    def kv_copy_z(way, u, src, steps):
        return remote(src, kv.at[u, way], zsend.at[0, way, u], zrecv.at[0, way, u], along_z(steps))

    def kv_first(way, u):
        steps = -u if way == 0 else u + 1
        return kv_copy_z(way, u, kv.at[0, 0], steps), wanted(way, u, steps)

    def kv_onward(way, u):
        steps = -2 if way == 0 else 2
        return kv_copy_z(way, u, kv.at[lax.max(u - 2, 0), way], steps), wanted(way, u, steps)

    def kv_start():
        for way, u in ((1, 1), (0, 2), (1, 0), (0, 1)):
            copy, needed = kv_first(way, u)
            pl.when(needed)(copy.start)

    def kv_take(u):
        for way in (1, 0):

            @pl.when(wanted(way, u, 0) & ((u > 0) | (way == 1)))
            def _():
                kv_onward(way, u)[0].wait_recv()

            copy, needed = kv_onward(way, u + 2)
            pl.when(needed & (u + 2 < units) & ((u > 0) | (way == 1)))(copy.start)

    def kv_drain(u):
        for way in (0, 1):
            steps = (-1 if way == 0 else 1) * jnp.minimum(u + way, 2)
            pl.when(wanted(way, u, steps) & ((u > 0) | (way == 1)))(kv_onward(way, u)[0].wait_send)

    for d in range(1, nx):
        kv_copy(d).wait_recv()
    kv_start()
    for d in range(1, nx):
        q_copy(d).wait_recv()

    mine = nx * count
    per = q_width // HD
    limit = seq_length[0]
    top_score[...] = jnp.full(top_score.shape, masked, f32)
    weight_sum[...] = jnp.zeros(weight_sum.shape, f32)
    mixed_values[...] = jnp.zeros(mixed_values.shape, f32)
    q_row = lax.broadcasted_iota(jnp.int32, (per * mine, 2 * mine), 0)
    k_row = lax.broadcasted_iota(jnp.int32, (per * mine, 2 * mine), 1)
    q_pos = z * mine + lax.rem(q_row, mine)

    def attend(u, carry):
        kv_take(u)
        q = jnp.concatenate(
            [q_all[:, :, j * HD : (j + 1) * HD].reshape(mine, HD) for j in range(per)], axis=0
        )
        k = kv[u, :, :, :, :HD].reshape(2 * mine, HD)
        v = kv[u, :, :, :, HD:].reshape(2 * mine, HD)
        s = lax.dot_general(q, k, (((1,), (1,)), ((), ())), preferred_element_type=f32) * (1.0 / math.sqrt(HD))
        k_pos = jnp.where(
            k_row < mine, lax.rem(z + u, nz) * mine + k_row, lax.rem(z - u - 1 + nz, nz) * mine + k_row - mine
        )
        allowed = (k_pos <= q_pos) & (k_pos < limit)
        s = jnp.where(allowed, s, masked)
        old = top_score[:, 0:1]
        new = jnp.maximum(old, jnp.max(s, axis=1, keepdims=True))
        p = jnp.where(allowed, jnp.exp(s - new), 0.0)
        keep = jnp.exp(old - new)
        top_score[...] = jnp.broadcast_to(new, top_score.shape)
        weight_sum[...] = weight_sum[...] * keep + lane_sum(p)
        mixed_values[...] = mixed_values[...] * keep + jnp.dot(p.astype(bf16), v, preferred_element_type=f32)
        return carry

    for u in range(units):
        attend(u, 0)
    ahead = chunks - 3
    for k in range(ahead):
        weight_copy(k).start()
    attended = mixed_values[...] / weight_sum[...]
    for s in range(nx):
        for j in range(per):
            piece = attended[j * mine + s * count : j * mine + (s + 1) * count]
            att_out[s, :, j * HD : (j + 1) * HD] = piece.astype(bf16)
    att_in[x] = att_out[x]
    for d in far_first:
        att_copy(d).start()
    for d in range(1, nx):
        kv_copy(d).wait_send()
        q_copy(d).wait_send()
    for d in range(1, nx):
        att_copy(d).wait_recv()
    for s in range(nx):
        at = slice(s * q_width, (s + 1) * q_width)
        hidden[:, at] = stream[:, at].astype(f32) + att_in[s].astype(f32)

    def both(index, message):
        stats[index] = message
        copy = remote(stats.at[index], stats_in.at[index], tsend.at[index], trecv.at[index], twin)
        copy.start()
        copy.wait()
        return message + stats_in[index]

    lane = lax.broadcasted_iota(jnp.int32, (count, META), 1)
    row = lax.broadcasted_iota(jnp.int32, (count, META), 0)

    def upright(line):
        return lane_sum(jnp.where(lane == row, jnp.broadcast_to(line, (count, META)), 0.0))

    h_all = hidden[...]
    gained = h_all * norm_gain[...]
    message = jnp.where(lane == EXPERTS, lane_sum(h_all * h_all), 0.0)
    for e in range(EXPERTS):
        message = jnp.where(lane == e, lane_sum(gained * router[e : e + 1]), message)
    total = both(0, message)
    sq = lane_sum(jnp.where(lane == EXPERTS, total, 0.0))
    scale = lax.rsqrt(sq / full_width + eps)
    logits = total * scale
    spread = jnp.concatenate([routes[...].astype(f32), jnp.zeros((2, META - count), f32)], axis=1)
    first, second = upright(spread[0:1]).astype(jnp.int32), upright(spread[1:2]).astype(jnp.int32)
    hit_a, hit_b = lane == first, lane == second
    gap = lane_sum(jnp.where(hit_a, logits, 0.0)) - lane_sum(jnp.where(hit_b, logits, 0.0))
    gate_a, gate_b = 1.0 / (1.0 + jnp.exp(-gap)), 1.0 / (1.0 + jnp.exp(gap))
    hits = jnp.where(hit_a | hit_b, 1.0, 0.0)
    rank = jnp.zeros((count, META), f32)
    for i in range(count - 1):
        rank = rank + jnp.where(row > i, jnp.broadcast_to(hits[i : i + 1], (count, META)), 0.0)
    place = jnp.where(hits > 0.5, rank + 1.0, 0.0)
    normed = gained * scale
    low, high = normed[:, :narrow], normed[:, narrow:]
    rows_out[:, :narrow] = jnp.where(c == 0, high, low).astype(bf16)
    rows_out[:, narrow:] = place.astype(bf16)
    rows_z[0, c, :, :narrow] = jnp.where(c == 0, low, high).astype(bf16)
    rows_z[0, c, :, narrow:] = place.astype(bf16)

    def mate_rows():
        return remote(rows_out, rows_z.at[0, c], zsend.at[1, 0, 0], zrecv.at[1, 0, 0], mate)

    def rows_copy(b, u):
        return remote(
            rows_z.at[lax.max(u - 2, 0), b], rows_z.at[u, b], zsend.at[1, b, u], zrecv.at[1, b, u],
            along_z(2 - 4 * lax.rem(u, 2)),
        )

    mate_rows().start()

    def rows_take(u):
        @pl.when(u == 0)
        def _():
            mate_rows().wait_recv()
            for b in (0, 1):
                rows_copy(b, 1).start()
                rows_copy(b, 2).start()

        @pl.when(u > 0)
        def _():
            for b in (0, 1):
                rows_copy(b, u).wait_recv()

                @pl.when(u + 2 < units)
                def _():
                    rows_copy(b, u + 2).start()

    def rows_drain(u):
        @pl.when(u == 0)
        def _():
            mate_rows().wait_send()

        @pl.when(u > 0)
        def _():
            for b in (0, 1):
                rows_copy(b, u).wait_send()

    info[0] = place
    info[1] = jnp.where(hit_a, gate_a, jnp.where(hit_b, gate_b, 0.0))

    ringed, chained = units, units
    my_expert = z // (nz // EXPERTS)
    slots = count // 2

    def column(table, expert):
        return lane_sum(jnp.where(lane == expert, table, 0.0))

    def choose(u):
        out = jnp.zeros((count, narrow), f32)
        for half in (0, 1):
            block = rows_z[u, half].astype(f32)
            places = jnp.broadcast_to(column(block[:, narrow:], my_expert), (count, META))
            for i in range(count):
                want = jnp.broadcast_to(places[i : i + 1], (count, META)) + (slots * half)
                chosen = jnp.where(((row + 1).astype(f32) == want) & (want > slots * half + 0.5), 1.0, 0.0)
                out = out + chosen[:, 0:1] * block[i : i + 1, :narrow]
        rows_x[u, x] = out.astype(bf16)

    def g_copy(way, u, h):
        back = nx - (h - 1) if way == 0 else h - 1
        at = rows_x.at[u, lax.rem(x + back, nx)]
        return remote(
            at, at, xsend.at[0, way, u, h - 1], xrecv.at[0, way, u, h - 1], right if way == 0 else left
        )

    def ups_copy(u):
        return remote(ups_out.at[u], ups_in.at[0, u], usend.at[0, u], urecv.at[0, u], mate)

    def cross_copy(u):
        return remote(ups_out.at[u], ups_in.at[1, u], usend.at[3, u], urecv.at[3, u], diagonal)

    def twin_copy(u):
        return remote(ups.at[u], ups_twin.at[u], usend.at[1, u], urecv.at[1, u], twin)

    def project(u):
        got = rows_x[u].reshape(mine, narrow)
        ups_out[u] = jnp.dot(got, w_up_in[...], preferred_element_type=f32).astype(bf16)
        ups_copy(u).start()
        cross_copy(u).start()
        ups[u] = jnp.dot(got, w_up[...], preferred_element_type=f32)
        twin_copy(u).start()

    def way_of(d):
        return (0, d) if d <= hops else (1, nx - d)

    def wide_copy(u, d):
        way, h = way_of(d)
        at = rows_x.at[u, x]
        return remote(
            at, at, xsend.at[0, way, u, h - 1], xrecv.at[0, way, u, h - 1], {"x": lax.rem(x + d, nx)}
        )

    def part_copy(u, d):
        way, h = way_of(d)
        peer = lax.rem(x + d, nx)
        return remote(
            parts.at[u, peer], recv.at[way, u, h - 1], xsend.at[1, way, u, h - 1], xrecv.at[1, way, u, h - 1],
            {"x": peer},
        )

    def own(way, u, k):
        ahead = hops - k
        return parts.at[u, lax.rem(x + (ahead if way == 0 else nx - ahead), nx)]

    def r_copy(way, u, k, src):
        return remote(
            src, recv.at[way, u, k], xsend.at[1, way, u, k], xrecv.at[1, way, u, k], right if way == 0 else left
        )

    def expand(u):
        ups_copy(u).wait_recv()
        cross_copy(u).wait_recv()
        twin_copy(u).wait_recv()
        v = ups[u] + ups_twin[u] + (ups_in[0, u].astype(f32) + ups_in[1, u].astype(f32))
        active = (v / (1.0 + jnp.exp(-v))).astype(bf16)
        made = jnp.dot(active, w_down[...], preferred_element_type=f32)
        for d in range(nx):
            parts[u, d] = made[d * count : (d + 1) * count].astype(bf16)

        @pl.when(u < chained)
        def _():
            for way in (0, 1):

                @pl.when(lax.rem(u, 2) == way)
                def _():
                    r_copy(way, u, 0, own(way, u, 0)).start()

        @pl.when(u >= chained)
        def _():
            for d in far_first:
                part_copy(u, d).start()

    def offset(u):
        return ((u + 1) // 2) * (2 * lax.rem(u, 2) - 1)

    def back_copy(b, u):
        to = {"z": 2 * lax.rem(m + offset(u) + pairs, pairs) + b}
        return remote(back_out.at[u, b], back_in.at[u, c], bsend.at[b, u], brecv.at[c, u], to)

    def back_arrival(b, u):
        to = {"z": 2 * lax.rem(m + offset(u) + pairs, pairs) + b}
        return remote(back_out.at[u, b], back_in.at[u, b], bsend.at[b, u], brecv.at[b, u], to)

    def home(u):
        def settle(total):
            done = total.astype(bf16)
            back_in_or_out(u, done)

        @pl.when(u < chained)
        def _():
            for way in (0, 1):
                r_copy(way, u, hops - 1, own(way, u, hops - 1)).wait_recv()
            both_ways = recv[0, u, hops - 1].astype(f32) + recv[1, u, hops - 1].astype(f32)
            settle(parts[u, x].astype(f32) + both_ways)

        @pl.when(u >= chained)
        def _():
            total = parts[u, x].astype(f32)
            for d in range(1, nx):
                part_copy(u, d).wait_recv()
                way, h = way_of(d)
                total = total + recv[way, u, h - 1].astype(f32)
            settle(total)

    def back_in_or_out(u, done):
        for b in (0, 1):
            back_out[u, b] = done[b * slots : (b + 1) * slots]

            @pl.when((u > 0) | (c != b))
            def _():
                back_copy(b, u).start()

            @pl.when((u == 0) & (c == b))
            def _():
                back_in[0, b] = done[b * slots : (b + 1) * slots]

    def blend(u):
        source = lax.rem(m - offset(u) + pairs, pairs)
        expert = 2 * source // (nz // EXPERTS)
        places, gate = column(info[0], expert), column(info[1], expert)
        weights = [jnp.where(places == float(i + 1), gate, 0.0) for i in range(slots)]
        for b in (0, 1):

            @pl.when((u > 0) | (c != b))
            def _():
                back_arrival(b, u).wait_recv()

            got = back_in[u, b].astype(f32)
            mix = hidden[...]
            for i in range(slots):
                mix = mix + weights[i] * got[i : i + 1]
            hidden[...] = mix

    for d in range(1, nx):
        att_copy(d).wait_send()
    up_copy.wait()
    down_copy.wait()
    groups = ((0, units, hops, hops),)

    def staged(step, delay, work):
        for low, high, start, end in groups:
            u = step - start - (delay if delay < 2 else delay - 1 + end)
            pl.when((u >= low) & (u < high))(functools.partial(work, u))

    def collect(u):
        @pl.when(u < ringed)
        def _():
            for way in (0, 1):

                @pl.when(lax.rem(u, 2) == way)
                def _():
                    g_copy(way, u, hops).wait_recv()

        @pl.when(u >= ringed)
        def _():
            for d in range(1, nx):
                way, h = way_of(d)
                g_copy(way, u, h).wait_recv()

        project(u)

    first_project = min(hops, ringed + 1)

    def slot(step, carry):
        @pl.when(step < units)
        def _():
            rows_take(step)
            choose(step)

            @pl.when(step == units - 1)
            def _():
                for d in range(1, nz):
                    greet(along_z(d))

            @pl.when(step < ringed)
            def _():
                g_copy(0, step, 1).start()
                g_copy(1, step, 1).start()

            @pl.when(step >= ringed)
            def _():
                for d in far_first:
                    wide_copy(step, d).start()

        for k in range(ahead, chunks):

            @pl.when(step == max(0, first_project - 4) + k - ahead)
            def _():
                weight_copy(k).start()

        for h in range(1, hops):
            u = step - h

            @pl.when((u >= 0) & (u < ringed))
            def _():
                for way in (0, 1):
                    g_copy(way, u, h).wait_recv()
                    if h < hops - 1:
                        g_copy(way, u, h + 1).start()
                    else:

                        @pl.when(lax.rem(u, 2) == way)
                        def _():
                            g_copy(way, u, h + 1).start()

        for k in range(1, hops):
            u = step - hops - 1 - k

            @pl.when((u >= 0) & (u < chained))
            def _():
                for way in (0, 1):

                    def add():
                        r_copy(way, u, k - 1, own(way, u, k - 1)).wait_recv()
                        total = recv[way, u, k - 1].astype(f32) + own(way, u, k)[...].astype(f32)
                        sums[way, u, k] = total.astype(bf16)
                        r_copy(way, u, k, sums.at[way, u, k]).start()

                    if k > 1:
                        add()
                    else:
                        pl.when(lax.rem(u, 2) == way)(add)

                        @pl.when(lax.rem(u, 2) != way)
                        def _():
                            r_copy(way, u, k, own(way, u, k)).start()

        first_home = min(low + start + 1 + end for low, high, start, end in groups)

        @pl.when(step == first_home)
        def _():
            pl.semaphore_wait(barrier, nz - 1)

        @pl.when(step == first_project)
        def _():
            for k in range(chunks):
                weight_copy(k).wait_recv()

        staged(step, 0, collect)
        staged(step, 1, expand)
        staged(step, 2, home)
        staged(step, 6, blend)
        return carry

    last = max(high - 1 + start + 5 + end for low, high, start, end in groups)
    lax.fori_loop(0, last + 1, slot, 0)
    out = hidden[...]
    layer_out[...] = out.astype(bf16)
    message = jnp.where(lane == 0, lane_sum(out * out), 0.0)
    message = jnp.where(lane == 1, lane_sum(out * (final_gain[...] * value_weight[...])), message)
    total = both(1, message)
    estimate = total[:, 1:2] * lax.rsqrt(total[:, 0:1] / full_width + eps) + value_bias[0]
    real = (z * nx + x) * count + row < limit
    flat = jnp.sum(jnp.where((lane == row) & real, estimate, 0.0), axis=0, keepdims=True)
    values[...] = flat

    def drain(u, carry):
        kv_drain(u)
        rows_drain(u)
        ups_copy(u).wait_send()
        twin_copy(u).wait_send()
        cross_copy(u).wait_send()
        for b in (0, 1):

            @pl.when((u > 0) | (c != b))
            def _():
                back_copy(b, u).wait_send()

        for way in (0, 1):
            even = lax.rem(u, 2) == way
            for k in range(1, hops):
                g_copy(way, u, k).wait_send()
            for k in range(1, hops if way == 0 else hops - 1):
                r_copy(way, u, k, own(way, u, k)).wait_send()
            one_way = (u < ringed) & even
            pl.when(one_way | (u >= ringed) if way == 0 else one_way)(g_copy(way, u, hops).wait_send)
            pl.when(((u < chained) & even) | (u >= chained))(r_copy(way, u, 0, own(way, u, 0)).wait_send)
            if way == 1:
                pl.when(u < chained)(r_copy(way, u, hops - 1, own(way, u, hops - 1)).wait_send)

        return carry

    lax.fori_loop(0, units, drain, 0)
    for k in range(chunks):
        weight_copy(k).wait_send()


def on_device(dims, *args):
    (stream, queries, key_rows, value_rows, routes, seq_length, norm_gain, router) = args[:8]
    (w_up, w_down, final_gain, value_weight, value_bias) = args[8:]
    nz, nx, _ = dims
    units, hops = nz // 2, nx // 2
    count, width = stream.shape
    hid, narrow = w_up.shape[1], width // 2
    heads = key_rows.shape[1] // HD
    mine = nx * count
    stacked = width // nx // HD * mine
    vmem, smem, far = (
        pl.BlockSpec(memory_space=pltpu.VMEM),
        pl.BlockSpec(memory_space=pltpu.SMEM),
        pl.BlockSpec(memory_space=pl.ANY),
    )
    dma = pltpu.SemaphoreType.DMA
    layer_out, values = pl.pallas_call(
        functools.partial(kernel, dims),
        out_shape=(
            jax.ShapeDtypeStruct((count, width), bf16),
            jax.ShapeDtypeStruct((1, META), f32),
        ),
        in_specs=[vmem, vmem, vmem, vmem, vmem, smem, vmem, vmem, far, far, vmem, vmem, smem],
        out_specs=(vmem, vmem),
        scratch_shapes=[
            pltpu.VMEM((nx, count, width // nx), bf16),
            pltpu.VMEM((heads, count, 2 * HD), bf16),
            pltpu.VMEM((units, 2, nx, count, 2 * HD), bf16),
            pltpu.VMEM((nx, count, width // nx), bf16),
            pltpu.VMEM((nx, count, width // nx), bf16),
            pltpu.VMEM((stacked, HD), f32),
            pltpu.VMEM((stacked, HD), f32),
            pltpu.VMEM((stacked, HD), f32),
            pltpu.VMEM((count, narrow + META), bf16),
            pltpu.VMEM((units, 2, count, narrow + META), bf16),
            pltpu.VMEM((units, nx, count, narrow), bf16),
            pltpu.VMEM((count, width), f32),
            pltpu.VMEM((2, count, META), f32),
            pltpu.VMEM((narrow, hid), bf16),
            pltpu.VMEM((hid, width), bf16),
            pltpu.VMEM((narrow, hid), bf16),
            pltpu.VMEM((2, count, META), f32),
            pltpu.VMEM((2, count, META), f32),
            pltpu.VMEM((units, mine, hid), f32),
            pltpu.VMEM((units, mine, hid), bf16),
            pltpu.VMEM((2, units, mine, hid), bf16),
            pltpu.VMEM((units, mine, hid), f32),
            pltpu.VMEM((units, nx, count, width), bf16),
            pltpu.VMEM((2, units, hops, count, width), bf16),
            pltpu.VMEM((2, units, hops, count, width), bf16),
            pltpu.VMEM((units, 2, count // 2, width), bf16),
            pltpu.VMEM((units, 2, count // 2, width), bf16),
            dma((2,)),
            dma((3, nx)),
            dma((3, nx)),
            dma((2, 2, units)),
            dma((2, 2, units)),
            dma((2, 2, units, hops)),
            dma((2, 2, units, hops)),
            dma((2, units)),
            dma((2, units)),
            dma((2,)),
            dma((2,)),
            dma((4, units)),
            dma((4, units)),
            dma((chunks,)),
            dma((chunks,)),
        ],
        compiler_params=pltpu.CompilerParams(
            collective_id=0, has_side_effects=True, vmem_limit_bytes=56 * 2**20
        ),
        name="layer",
    )(
        queries,
        key_rows,
        value_rows,
        stream,
        routes.T,
        seq_length,
        norm_gain.reshape(1, width),
        router.T,
        w_up,
        w_down,
        final_gain.reshape(1, width),
        value_weight.reshape(1, width),
        value_bias,
    )
    return layer_out, values[0, :count]


def build(mesh, nz, nx, full_width):
    finer = Mesh(
        mesh.devices.reshape(mesh.shape["groups"], nz, nx, mesh.shape["tp"]),
        ("groups", "z", "x", "tp"),
    )
    placed = (
        P(GROUPS_SEQ, "tp"),
        P(GROUPS_SEQ, "tp"),
        P(GROUPS_SEQ, "tp"),
        P(GROUPS_SEQ, "tp"),
        P(GROUPS_SEQ, None),
        P("groups"),
        P("tp"),
        P("tp", None),
        P("tp", SEQ),
        P(SEQ, "tp"),
        P("tp"),
        P("tp"),
        P(),
    )
    return jax.shard_map(
        functools.partial(on_device, (nz, nx, full_width)),
        mesh=finer,
        in_specs=placed,
        out_specs=(P(GROUPS_SEQ, "tp"), P(GROUPS_SEQ)),
        check_vma=False,
    )


def solution(mesh):
    return build(mesh, 16, mesh.shape["seq"] // 16, 6144)
```
